16 devices in a mesh: dp: 2 (over y, z), sp: 8 (over x, core).
Axes of the slice: x: 4, y: 2, z: 1, core: 2. Of those that a mesh axis runs over, the one named last changes fastest.
The devices are a block of a 4x4x8 slice.
Arguments:
- x_in: bfloat16 [4, 3072, 2048], P('dp', 'sp'), parts along dimension 0
- d_out: bfloat16 [4, 3072, 2048], P('dp', 'sp'), parts along dimension 0
- gain: float32 [2048], replicated
- w_q: bfloat16 [2048, 32, 64], replicated
- w_k: bfloat16 [2048, 8, 64], replicated
- w_v: bfloat16 [2048, 8, 64], replicated
- w_o: bfloat16 [32, 64, 2048], replicated
Outputs:
- output 1: bfloat16 [4, 3072, 2048], P('dp', 'sp'), parts along dimension 0
- output 2: bfloat16 [4, 3072, 2048], P('dp', 'sp'), parts along dimension 0
- output 3: float32 [4096, 32, 64], P('dp'), parts along dimension 0
- output 4: float32 [4096, 8, 64], P('dp'), parts along dimension 0
- output 5: float32 [4096, 8, 64], P('dp'), parts along dimension 0
- output 6: float32 [64, 64, 2048], P('dp'), parts along dimension 0
- output 7: float32 [4096], P('dp'), parts along dimension 0
There are 2 independent parts. The reference program is written for one: setup_inputs(seed, part) draws one part's arguments, and reference() takes and returns one part's arrays. A program takes and returns all parts, laid end to end along the dimension named above; an argument that names none is the same for every part.
All inputs are finite; a program needn't handle non-finite values.
Results may differ from the reference program's by a relative error of at most 0.0124358.
Values are sent between devices in bfloat16 or wider.
A program may use at most 768 MiB of HBM per device.

```python
import jax
import jax.numpy as jnp
from jax import lax

BATCH = 2
SEQ = 3072
D_MODEL = 2048
HEADS = 32
KV_HEADS = 8
HEAD = 64

ROPE_BASE = 1000000.0
NORM_EPS = 1e-5


def setup_inputs(seed: int = 0, part: int = 0) -> dict:
    part_key = jax.random.fold_in(jax.random.key(seed), part)
    key_x, key_dy = jax.random.split(part_key, 2)
    shared = jax.random.split(jax.random.key(seed + 1), 5)
    x_val = jax.random.normal(key_x, (BATCH, SEQ, D_MODEL), jnp.float32)
    dy_val = jax.random.normal(key_dy, (BATCH, SEQ, D_MODEL), jnp.float32)
    gain = jax.random.uniform(shared[0], (D_MODEL,), jnp.float32, 0.6, 1.4)
    in_scale = D_MODEL ** -0.5
    w_q = jax.random.normal(shared[1], (D_MODEL, HEADS, HEAD), jnp.float32) * (1.5 * in_scale)
    w_k = jax.random.normal(shared[2], (D_MODEL, KV_HEADS, HEAD), jnp.float32) * (1.5 * in_scale)
    w_v = jax.random.normal(shared[3], (D_MODEL, KV_HEADS, HEAD), jnp.float32) * in_scale
    w_o = jax.random.normal(shared[4], (HEADS, HEAD, D_MODEL), jnp.float32) * (2.0 * (HEADS * HEAD) ** -0.5)
    return {'x_in': x_val.astype(jnp.bfloat16), 'd_out': dy_val.astype(jnp.bfloat16), 'gain': gain, 'w_q': w_q.astype(jnp.bfloat16), 'w_k': w_k.astype(jnp.bfloat16), 'w_v': w_v.astype(jnp.bfloat16), 'w_o': w_o.astype(jnp.bfloat16)}


def rope_tables(positions):
    half = HEAD // 2
    inv_freq = ROPE_BASE ** (-2.0 * jnp.arange(half, dtype=jnp.float32) / HEAD)
    angle = positions[:, None] * inv_freq[None, :]
    return jnp.cos(angle), jnp.sin(angle)


def rotate(t_val, cos_t, sin_t):
    half = HEAD // 2
    first = t_val[..., :half]
    second = t_val[..., half:]
    cos_b = cos_t[:, None, :]
    sin_b = sin_t[:, None, :]
    return jnp.concatenate([first * cos_b - second * sin_b, second * cos_b + first * sin_b], axis=-1)


def attention(q_all, k_all, v_all):
    group = HEADS // KV_HEADS
    block_len = 128
    num_blocks = SEQ // block_len
    scale = HEAD ** -0.5
    k_f32 = k_all.astype(jnp.float32)
    v_f32 = v_all.astype(jnp.float32)
    q_grouped = jnp.moveaxis(q_all.reshape(BATCH, num_blocks, block_len, KV_HEADS, group, HEAD), 1, 0)
    key_pos = jnp.arange(SEQ)

    def one_block(pair):
        q_rows, block_idx = pair
        scores = jnp.einsum('bqkgd,btkd->bkgqt', q_rows.astype(jnp.float32), k_f32) * scale
        q_pos = block_idx * block_len + jnp.arange(block_len)
        scores = jnp.where(key_pos[None, :] <= q_pos[:, None], scores, -1e30)
        attn_weights = jax.nn.softmax(scores, axis=-1).astype(jnp.bfloat16).astype(jnp.float32)
        out_rows = jnp.einsum('bkgqt,btkd->bqkgd', attn_weights, v_f32)
        return out_rows.astype(jnp.bfloat16)

    out_blocks = lax.map(jax.checkpoint(one_block), (q_grouped, jnp.arange(num_blocks)))
    return jnp.moveaxis(out_blocks, 0, 1).reshape(BATCH, SEQ, HEADS, HEAD)


def block_forward(x_in, gain, w_q, w_k, w_v, w_o):
    x_f32 = x_in.astype(jnp.float32)
    inv_rms = lax.rsqrt(jnp.mean(x_f32 * x_f32, axis=-1, keepdims=True) + NORM_EPS)
    normed = (x_f32 * inv_rms * gain).astype(jnp.bfloat16).astype(jnp.float32)
    cos_t, sin_t = rope_tables(jnp.arange(SEQ, dtype=jnp.float32))
    q_all = rotate(jnp.einsum('btd,dhe->bthe', normed, w_q), cos_t, sin_t).astype(jnp.bfloat16)
    k_all = rotate(jnp.einsum('btd,dhe->bthe', normed, w_k), cos_t, sin_t).astype(jnp.bfloat16)
    v_all = jnp.einsum('btd,dhe->bthe', normed, w_v).astype(jnp.bfloat16)
    mixed = attention(q_all, k_all, v_all)
    y_proj = jnp.einsum('bthe,hed->btd', mixed.astype(jnp.float32), w_o)
    return (x_f32 + y_proj).astype(jnp.bfloat16)


def reference(x_in, d_out, gain, w_q, w_k, w_v, w_o):
    y_out, pullback = jax.vjp(block_forward, x_in, gain, w_q.astype(jnp.float32), w_k.astype(jnp.float32), w_v.astype(jnp.float32), w_o.astype(jnp.float32))
    d_x, d_gain, d_wq, d_wk, d_wv, d_wo = pullback(d_out)
    return (y_out, d_x, d_wq, d_wk, d_wv, d_wo, d_gain)
```

```python
import functools
import math
import jax
import jax.numpy as jnp
from jax import lax
from jax.experimental import pallas as pl
from jax.experimental.pallas import tpu as pltpu
from jax.sharding import PartitionSpec as P

ROPE_BASE = 1000000.0
NORM_EPS = 1e-5
LOG2E = math.log2(math.e)
NEG = -1e30
F32 = jnp.float32
BF16 = jnp.bfloat16

NN = (((1,), (0,)), ((), ()))
NT = (((1,), (1,)), ((), ()))
TN = (((0,), (0,)), ((), ()))


def dot(a, b, dims=NN):
    return lax.dot_general(a, b, dims, preferred_element_type=F32)


def rope_tables_t(seq_len, head_dim):
    half = head_dim // 2
    inv_freq = ROPE_BASE ** (-2.0 * jnp.arange(half, dtype=F32) / head_dim)
    angle = jnp.arange(seq_len).astype(F32)[None, :] * inv_freq[:, None]
    return jnp.cos(angle), jnp.sin(angle)


def norm_forward(x_local, gain):
    x_f32 = x_local.astype(F32)
    inv_rms = lax.rsqrt(jnp.mean(x_f32 * x_f32, axis=-1, keepdims=True) + NORM_EPS)
    x_hat = x_f32 * inv_rms
    return x_hat, inv_rms, (x_hat * gain).astype(BF16)


def norm_backward(d_normed, x_hat, inv_rms, gain):
    d_hat = d_normed * gain
    return inv_rms * (d_hat - x_hat * jnp.mean(d_hat * x_hat, axis=-1, keepdims=True))


def project_kernel(group, dim, r_ref, w_ref, cos_ref, sin_ref, q_ref, k_ref, kt_ref, v_ref, vt_ref):
    half = dim // 2
    blk = r_ref.shape[1]
    lin = dot(w_ref[...], r_ref[0], NT)
    cos_t = cos_ref[...]
    sin_t = sin_ref[...]
    for h in range(group):
        a = lin[h * dim:h * dim + half]
        b = lin[h * dim + half:(h + 1) * dim]
        q_ref[0, :half, h * blk:(h + 1) * blk] = (a * cos_t - b * sin_t).astype(BF16)
        q_ref[0, half:, h * blk:(h + 1) * blk] = (b * cos_t + a * sin_t).astype(BF16)
    a = lin[group * dim:group * dim + half]
    b = lin[group * dim + half:(group + 1) * dim]
    v = lin[(group + 1) * dim:]
    kv = jnp.concatenate([a * cos_t - b * sin_t, b * cos_t + a * sin_t, v], axis=0)
    kt_ref[...] = kv[:dim].astype(BF16)
    vt_ref[...] = v.astype(BF16)
    kv_t = kv.T.astype(BF16)
    k_ref[...] = kv_t[:, :dim]
    v_ref[...] = kv_t[:, dim:]


def causal_mask(rows, cols, blk):
    key = lax.broadcasted_iota(jnp.int32, (rows, cols), 0)
    qry = lax.broadcasted_iota(jnp.int32, (rows, cols), 1) % blk
    return key <= qry


def forward_kernel(group, dim, q_ref, k_ref, vt_ref, o_ref, lse_ref, acc_ref, m_ref, l_ref):
    blk = o_ref.shape[2]
    i = pl.program_id(0)
    c2 = dim ** -0.5 * LOG2E
    acc_ref[...] = jnp.zeros_like(acc_ref)
    l_ref[...] = jnp.zeros_like(l_ref)
    m_ref[...] = jnp.full_like(m_ref, NEG)

    def tile(j, masked):
        off = pl.multiple_of(j * blk, blk)
        s = dot(k_ref[pl.ds(off, blk), :], q_ref[0])
        if masked:
            s = jnp.where(causal_mask(s.shape[0], s.shape[1], blk), s, NEG)
        m_old = m_ref[...]
        m_new = jnp.maximum(m_old, jnp.max(s, axis=0, keepdims=True) * c2)
        p = jnp.exp2(s * c2 - m_new)
        alpha = jnp.exp2(m_old - m_new)
        m_ref[...] = m_new
        l_ref[...] = l_ref[...] * alpha + jnp.sum(p, axis=0, keepdims=True)
        acc_ref[...] = acc_ref[...] * alpha + dot(vt_ref[:, pl.ds(off, blk)], p.astype(BF16))

    def step(j, carry):
        tile(j, False)
        return carry

    lax.fori_loop(0, i, step, 0)
    tile(i, True)
    l_val = l_ref[...]
    o = (acc_ref[...] * (1.0 / l_val)).astype(BF16)
    for h in range(group):
        o_ref[0, h * dim:(h + 1) * dim, :] = o[:, h * blk:(h + 1) * blk]
    lse_ref[0] = m_ref[...] + jnp.log2(l_val)


def out_grad_kernel(group, dim, first, *refs):
    if first:
        dy_ref, w_ref, o_ref, do_ref, dw_ref = refs
    else:
        dy_ref, w_ref, o_ref, prev_ref, do_ref, dw_ref = refs
    blk = dy_ref.shape[1]

    @pl.when(pl.program_id(0) == 0)
    def _():
        dw_ref[...] = jnp.zeros_like(dw_ref) if first else prev_ref[...]

    d_o = dot(w_ref[...], dy_ref[0], NT).astype(BF16)
    for h in range(group):
        do_ref[0, :, h * blk:(h + 1) * blk] = d_o[h * dim:(h + 1) * dim]
    dw_ref[...] += dot(o_ref[0], dy_ref[0])


def backward_kernel(group, dim, q_ref, do_ref, o_ref, lse_ref, k_ref, kt_ref, v_ref, cos_ref, sin_ref, out_ref,
                    dq_ref, dk_ref, dv_ref, delta_ref):
    blk = out_ref.shape[2]
    half = dim // 2
    step_id = pl.program_id(0)
    i = pl.num_programs(0) - 1 - step_id
    scale = dim ** -0.5
    c2 = scale * LOG2E

    @pl.when(step_id == 0)
    def _():
        dk_ref[...] = jnp.zeros_like(dk_ref)
        dv_ref[...] = jnp.zeros_like(dv_ref)

    dq_ref[...] = jnp.zeros_like(dq_ref)
    for h in range(group):
        prod = o_ref[0, h * dim:(h + 1) * dim, :].astype(F32) * do_ref[0, :, h * blk:(h + 1) * blk].astype(F32)
        delta_ref[:, h * blk:(h + 1) * blk] = jnp.sum(prod, axis=0, keepdims=True)

    def tile(j, masked):
        off = pl.multiple_of(j * blk, blk)
        s = dot(k_ref[pl.ds(off, blk), :], q_ref[0])
        p = jnp.exp2(s * c2 - lse_ref[0])
        if masked:
            p = jnp.where(causal_mask(s.shape[0], s.shape[1], blk), p, 0.0)
        dp = dot(v_ref[pl.ds(off, blk), :], do_ref[0]).astype(BF16).astype(F32)
        ds = (p * (dp - delta_ref[...])).astype(BF16)
        dv_ref[:, pl.ds(off, blk)] += dot(do_ref[0], p.astype(BF16), NT)
        dk_ref[:, pl.ds(off, blk)] += dot(q_ref[0], ds, NT)
        dq_ref[...] += dot(kt_ref[:, pl.ds(off, blk)], ds)

    def step(j, carry):
        tile(j, False)
        return carry

    lax.fori_loop(0, i, step, 0)
    tile(i, True)

    cos_t = cos_ref[...]
    sin_t = sin_ref[...]

    def rope_back(grad):
        grad = (grad * scale).astype(BF16).astype(F32)
        a = grad[:half]
        b = grad[half:]
        return (a * cos_t + b * sin_t).astype(BF16), (b * cos_t - a * sin_t).astype(BF16)

    for h in range(group):
        top, bottom = rope_back(dq_ref[:, h * blk:(h + 1) * blk])
        out_ref[0, h * dim:h * dim + half, :] = top
        out_ref[0, h * dim + half:(h + 1) * dim, :] = bottom
    off = pl.multiple_of(i * blk, blk)
    top, bottom = rope_back(dk_ref[:, pl.ds(off, blk)])
    base = group * dim
    out_ref[0, base:base + half, :] = top
    out_ref[0, base + half:base + dim, :] = bottom
    out_ref[0, base + dim:base + 2 * dim, :] = dv_ref[:, pl.ds(off, blk)].astype(BF16)


def weight_grad_kernel(first, *refs):
    if first:
        g_ref, r_ref, dw_ref = refs
    else:
        g_ref, r_ref, prev_ref, dw_ref = refs

    @pl.when(pl.program_id(0) == 0)
    def _():
        dw_ref[...] = jnp.zeros_like(dw_ref) if first else prev_ref[...]

    dw_ref[...] += dot(g_ref[0], r_ref[0])


def whole(*shape):
    return pl.BlockSpec(shape, lambda s: (0,) * len(shape))


def call(kernel, grid, in_specs, out_specs, out_shape, name, flops, scratch=(), aliases=None):
    return pl.pallas_call(
        kernel,
        grid=(grid,),
        in_specs=in_specs,
        out_specs=out_specs,
        out_shape=out_shape,
        scratch_shapes=list(scratch),
        input_output_aliases=aliases or {},
        name=name,
        cost_estimate=pl.CostEstimate(flops=int(flops), bytes_accessed=int(1e6), transcendentals=0),
        compiler_params=pltpu.CompilerParams(dimension_semantics=("arbitrary",)),
    )


def solution(mesh):
    seq_par = mesh.shape['sp']

    def local_step(x_local, dy_local, gain, w_q, w_k, w_v, w_o):
        batch, blk, d_model = x_local.shape
        num_q, dim = w_q.shape[1], w_q.shape[2]
        num_kv = w_k.shape[1]
        assert num_kv == seq_par
        group = num_q // num_kv
        half = dim // 2
        seq = blk * seq_par
        rows_q = group * dim
        rows = rows_q + 2 * dim
        cols = group * blk
        n = seq_par
        me = lax.axis_index('sp')

        wq_t = jnp.transpose(w_q, (1, 2, 0)).reshape(n, rows_q, d_model)
        wk_t = jnp.transpose(w_k, (1, 2, 0)).reshape(n, dim, d_model)
        wv_t = jnp.transpose(w_v, (1, 2, 0)).reshape(n, dim, d_model)
        wo_g = w_o.reshape(n, rows_q, d_model)
        w_all = jnp.concatenate([wq_t, wk_t, wv_t], axis=1)
        w_mine = lax.dynamic_index_in_dim(w_all, me, 0, keepdims=False)
        wo_mine = lax.dynamic_index_in_dim(wo_g, me, 0, keepdims=False)
        cos_t, sin_t = rope_tables_t(seq, dim)

        x_hat, inv_rms, normed = norm_forward(x_local, gain)
        r_all = [lax.all_gather(normed[b], 'sp', axis=0) for b in range(batch)]
        dy_all = [lax.all_gather(dy_local[b], 'sp', axis=0) for b in range(batch)]

        row3 = lambda a, b: pl.BlockSpec((1, a, b), lambda s: (s, 0, 0))
        lane = lambda a: pl.BlockSpec((a, blk), lambda s: (0, s))
        rev3 = lambda a, b: pl.BlockSpec((1, a, b), lambda s: (n - 1 - s, 0, 0))
        rev_lane = lambda a: pl.BlockSpec((a, blk), lambda s: (0, n - 1 - s))
        sds = jax.ShapeDtypeStruct
        tok = pl.BlockSpec((blk, dim), lambda s: (s, 0))
        mm = 2.0 * seq * d_model
        att = 2.0 * seq * seq * dim * group / 2

        project = call(functools.partial(project_kernel, group, dim), n,
                       [row3(blk, d_model), whole(rows, d_model), lane(half), lane(half)],
                       [row3(dim, cols), tok, lane(dim), tok, lane(dim)],
                       [sds((n, dim, cols), BF16), sds((seq, dim), BF16), sds((dim, seq), BF16),
                        sds((seq, dim), BF16), sds((dim, seq), BF16)], 'project', mm * rows)
        forward = call(functools.partial(forward_kernel, group, dim), n,
                       [row3(dim, cols), whole(seq, dim), whole(dim, seq)],
                       [row3(rows_q, blk), row3(1, cols)],
                       [sds((n, rows_q, blk), BF16), sds((n, 1, cols), F32)], 'forward', att * 8,
                       [pltpu.VMEM((dim, cols), F32), pltpu.VMEM((1, cols), F32), pltpu.VMEM((1, cols), F32)])
        backward = call(functools.partial(backward_kernel, group, dim), n,
                        [rev3(dim, cols), rev3(dim, cols), rev3(rows_q, blk), rev3(1, cols), whole(seq, dim),
                         whole(dim, seq), whole(seq, dim), rev_lane(half), rev_lane(half)],
                        rev3(rows, blk), sds((n, rows, blk), BF16), 'backward', att * 20,
                        [pltpu.VMEM((dim, cols), F32), pltpu.VMEM((dim, seq), F32), pltpu.VMEM((dim, seq), F32),
                         pltpu.VMEM((1, cols), F32)])

        def out_grad(dy_b, o_b, prev):
            first = prev is None
            args = (dy_b, wo_mine, o_b) + (() if first else (prev,))
            specs = [row3(blk, d_model), whole(rows_q, d_model), row3(rows_q, blk)]
            specs += [] if first else [whole(rows_q, d_model)]
            return call(functools.partial(out_grad_kernel, group, dim, first), n, specs,
                        [row3(dim, cols), whole(rows_q, d_model)],
                        [sds((n, dim, cols), BF16), sds((rows_q, d_model), F32)], 'out_grad', mm * rows_q * 2,
                        aliases=None if first else {3: 1})(*args)

        def weight_grad(g_b, r_b, prev):
            first = prev is None
            args = (g_b, r_b) + (() if first else (prev,))
            specs = [row3(rows, blk), row3(blk, d_model)] + ([] if first else [whole(rows, d_model)])
            return call(functools.partial(weight_grad_kernel, first), n, specs, whole(rows, d_model),
                        sds((rows, d_model), F32), 'weight_grad', mm * rows, aliases=None if first else {2: 0})(*args)

        swap = lambda t: lax.all_to_all(t, 'sp', 0, 0, tiled=True)
        heads, o_all, lse_all = [], [], []
        for b in range(batch):
            heads.append(project(r_all[b], w_mine, cos_t, sin_t))
            q_t, k, k_t, v, v_t = heads[b]
            o_b, lse_b = forward(q_t, k, v_t)
            o_all.append(o_b)
            lse_all.append(lse_b)
        o_local = [swap(o_all[b]).reshape(num_q * dim, blk) for b in range(batch)]
        d_wo_mine = None
        d_o = []
        for b in range(batch):
            do_b, d_wo_mine = out_grad(dy_all[b], o_all[b], d_wo_mine)
            d_o.append(do_b)
        d_wo = lax.all_gather(d_wo_mine, 'sp', axis=0, tiled=True)
        wo_flat = w_o.reshape(num_q * dim, d_model)
        y_proj = jnp.stack([dot(o_local[b], wo_flat, TN) for b in range(batch)])
        y_out = (x_local.astype(F32) + y_proj).astype(BF16)

        d_w_mine = None
        g_local = []
        for b in range(batch):
            q_t, k, k_t, v, v_t = heads[b]
            g_b = backward(q_t, d_o[b], o_all[b], lse_all[b], k, k_t, v, cos_t, sin_t)
            g_local.append(swap(g_b).reshape(n * rows, blk))
            d_w_mine = weight_grad(g_b, r_all[b], d_w_mine)
        d_wq = lax.all_gather(d_w_mine[:rows_q], 'sp', axis=0, tiled=True)
        d_wk = lax.all_gather(d_w_mine[rows_q:rows_q + dim], 'sp', axis=0, tiled=True)
        d_wv = lax.all_gather(d_w_mine[rows_q + dim:], 'sp', axis=0, tiled=True)

        w_flat = w_all.reshape(n * rows, d_model)
        d_normed = jnp.stack([dot(g_local[b], w_flat, TN) for b in range(batch)]).astype(BF16).astype(F32)
        d_x_norm = norm_backward(d_normed, x_hat, inv_rms, gain)
        d_gain = lax.psum(jnp.sum(d_normed * x_hat, axis=(0, 1)), 'sp')
        d_x = (dy_local.astype(F32) + d_x_norm).astype(BF16)
        back = lambda t, h: jnp.transpose(t.reshape(h, dim, d_model), (2, 0, 1))
        return (y_out, d_x, back(d_wq, num_q), back(d_wk, num_kv), back(d_wv, num_kv),
                d_wo.reshape(num_q, dim, d_model), d_gain)

    specs_in = (P('dp', 'sp', None), P('dp', 'sp', None), P(None), P(None, None, None), P(None, None, None), P(None, None, None), P(None, None, None))
    specs_out = (P('dp', 'sp', None), P('dp', 'sp', None), P('dp', None, None), P('dp', None, None), P('dp', None, None), P('dp', None, None), P('dp'))
    return jax.shard_map(local_step, mesh=mesh, in_specs=specs_in, out_specs=specs_out, check_vma=False)
```

```python
import functools
import math
import jax
import jax.numpy as jnp
from jax import lax
from jax.experimental import pallas as pl
from jax.experimental.pallas import tpu as pltpu
from jax.sharding import PartitionSpec as P

ROPE_BASE = 1000000.0
NORM_EPS = 1e-5
LOG2E = math.log2(math.e)
NEG = -1e30
F32 = jnp.float32
BF16 = jnp.bfloat16

MESH = pl.DeviceIdType.MESH
CORES = 2

NN = (((1,), (0,)), ((), ()))
NT = (((1,), (1,)), ((), ()))
TN = (((0,), (0,)), ((), ()))


def dot(a, b, dims=NN):
    return lax.dot_general(a, b, dims, preferred_element_type=F32)


def rope_tables_t(seq_len, head_dim):
    half = head_dim // 2
    inv_freq = ROPE_BASE ** (-2.0 * jnp.arange(half, dtype=F32) / head_dim)
    angle = jnp.arange(seq_len).astype(F32)[None, :] * inv_freq[:, None]
    return jnp.cos(angle), jnp.sin(angle)


def norm_forward(x_local, gain):
    x_f32 = x_local.astype(F32)
    inv_rms = lax.rsqrt(jnp.mean(x_f32 * x_f32, axis=-1, keepdims=True) + NORM_EPS)
    x_hat = x_f32 * inv_rms
    return x_hat, inv_rms, (x_hat * gain).astype(BF16)


def norm_backward(d_normed, x_hat, inv_rms, gain):
    d_hat = d_normed * gain
    return inv_rms * (d_hat - x_hat * jnp.mean(d_hat * x_hat, axis=-1, keepdims=True))


def remote(src, dst, send_sem, recv_sem, target):
    return pltpu.make_async_remote_copy(src_ref=src, dst_ref=dst, send_sem=send_sem, recv_sem=recv_sem,
                                        device_id={'sp': target}, device_id_type=MESH)


def enter(targets):
    barrier = pltpu.get_barrier_semaphore()
    for t in targets:
        pl.semaphore_signal(barrier, inc=1, device_id={'sp': t}, device_id_type=MESH)
    pl.semaphore_wait(barrier, len(targets))


class Ring:
    def __init__(self, n, src_ref, all_ref, send_sem, recv_sem):
        self.n, self.src, self.all, self.send_sem, self.recv_sem = n, src_ref, all_ref, send_sem, recv_sem
        me = lax.axis_index('sp')
        self.me, self.chip, self.core = me, me // CORES, me % CORES
        self.partner = self.at(0, 1 - self.core)

    def at(self, hop, core):
        chips = self.n // CORES
        return (self.chip + hop + chips) % chips * CORES + core

    def neighbours(self):
        return [self.partner] + [self.at(hop, core) for hop in (1, -1) for core in range(CORES)]

    def copy(self, src, slot, k, target):
        return remote(src, self.all.at[slot], self.send_sem.at[k], self.recv_sem.at[slot], target)

    def direct(self):
        out = [self.copy(self.src.at[1 - self.core], self.me, 0, self.partner)]
        k = 1
        for turn in range(CORES):
            for hop in (1, -1):
                core = (self.core + turn) % CORES
                out.append(self.copy(self.src.at[core], self.me, k, self.at(hop, core)))
                k += 1
        return out

    def relayed(self):
        first, second = self.at(-1, 0), self.at(1, 1)
        k = 1 + 2 * CORES
        return [self.copy(self.all.at[first], first, k, self.at(1, self.core)),
                self.copy(self.all.at[second], second, k + 1, self.at(-1, self.core))]

    def start(self):
        for c in self.direct():
            c.start()

    def relay(self):
        for c in self.relayed():
            c.start()

    def wait_block(self, slot):
        self.copy(self.all.at[slot], slot, 0, self.partner).wait_recv()

    def order(self):
        b, o = self.core, 1 - self.core
        return [self.me, self.partner, self.at(-1, b), self.at(1, b), self.at(-1, o), self.at(1, o),
                self.at(2, 0), self.at(2, 1)]

    def wait_sends(self):
        for c in self.direct() + self.relayed():
            c.wait_send()


RING_SENDS = 3 + 2 * CORES


def project_kernel(n, group, dim, r_hbm, w_ref, cos_ref, sin_ref, all_ref, q_ref, k_ref, kt_ref, v_ref, vt_ref,
                   block_ref, load_sem, send_sem, recv_sem):
    half = dim // 2
    blk = block_ref.shape[0]
    rows = (group + 2) * dim
    ring = Ring(n, r_hbm, all_ref, send_sem, recv_sem)
    enter(ring.neighbours())
    ring.start()
    order = ring.order()

    def body(p, carry):
        slot = order[0]
        for k in range(1, n):
            slot = jnp.where(p == k, order[k], slot)

        @pl.when(p == 0)
        def _():
            load = pltpu.make_async_copy(r_hbm.at[ring.core], block_ref, load_sem)
            load.start()
            load.wait()
            store = pltpu.make_async_copy(block_ref, all_ref.at[ring.me], load_sem)
            store.start()
            store.wait()

        for k in range(1, n):
            @pl.when(p == k)
            def _(k=k):
                if k == 4:
                    ring.wait_block(order[4])
                    ring.wait_block(order[5])
                    ring.relay()
                elif k != 5:
                    ring.wait_block(order[k])
                load = pltpu.make_async_copy(all_ref.at[order[k]], block_ref, load_sem)
                load.start()
                load.wait()

        off = pl.multiple_of(slot * blk, blk)
        cos_t = cos_ref[:, pl.ds(off, blk)]
        sin_t = sin_ref[:, pl.ds(off, blk)]
        for g in range(CORES):
            lin = dot(w_ref[g * rows:(g + 1) * rows], block_ref[...], NT)
            for h in range(group):
                a = lin[h * dim:h * dim + half]
                b = lin[h * dim + half:(h + 1) * dim]
                q_ref[g, slot, :half, h * blk:(h + 1) * blk] = (a * cos_t - b * sin_t).astype(BF16)
                q_ref[g, slot, half:, h * blk:(h + 1) * blk] = (b * cos_t + a * sin_t).astype(BF16)
            a = lin[group * dim:group * dim + half]
            b = lin[group * dim + half:(group + 1) * dim]
            v = lin[(group + 1) * dim:]
            kv = jnp.concatenate([a * cos_t - b * sin_t, b * cos_t + a * sin_t, v], axis=0)
            kt_ref[g, :, pl.ds(off, blk)] = kv[:dim].astype(BF16)
            vt_ref[g, :, pl.ds(off, blk)] = v.astype(BF16)
            kv_t = kv.T.astype(BF16)
            k_ref[g, pl.ds(off, blk), :] = kv_t[:, :dim]
            v_ref[g, pl.ds(off, blk), :] = kv_t[:, dim:]
        return carry

    lax.fori_loop(0, n, body, 0)
    ring.wait_sends()


def causal_mask(rows, cols, blk):
    key = lax.broadcasted_iota(jnp.int32, (rows, cols), 0)
    qry = lax.broadcasted_iota(jnp.int32, (rows, cols), 1) % blk
    return key <= qry


def forward_kernel(n, group, dim, relay_at, q_ref, k_ref, vt_ref, dy_hbm, o_ref, lse_ref, all_ref, acc_ref, m_ref, l_ref,
                   bounce_ref, load_sem, send_sem, recv_sem):
    blk = o_ref.shape[2]
    step_id = pl.program_id(0)
    i = step_id % n
    c2 = dim ** -0.5 * LOG2E
    ring = Ring(n, dy_hbm, all_ref, send_sem, recv_sem)
    order = ring.order()

    @pl.when(step_id == 0)
    def _():
        enter(ring.neighbours())
        ring.start()
        load = pltpu.make_async_copy(dy_hbm.at[ring.core], bounce_ref, load_sem)
        load.start()
        load.wait()
        store = pltpu.make_async_copy(bounce_ref, all_ref.at[ring.me], load_sem)
        store.start()
        store.wait()

    @pl.when(step_id == relay_at)
    def _():
        ring.wait_block(order[4])
        ring.wait_block(order[5])
        ring.wait_block(order[2])
        ring.wait_block(order[3])
        ring.relay()

    acc_ref[...] = jnp.zeros_like(acc_ref)
    l_ref[...] = jnp.zeros_like(l_ref)
    m_ref[...] = jnp.full_like(m_ref, NEG)

    def tile(j, masked):
        off = pl.multiple_of(j * blk, blk)
        s = dot(k_ref[0, pl.ds(off, blk), :], q_ref[0, 0])
        if masked:
            s = jnp.where(causal_mask(s.shape[0], s.shape[1], blk), s, NEG)
        m_old = m_ref[...]
        m_new = jnp.maximum(m_old, jnp.max(s, axis=0, keepdims=True) * c2)
        p = jnp.exp2(s * c2 - m_new)
        alpha = jnp.exp2(m_old - m_new)
        m_ref[...] = m_new
        l_ref[...] = l_ref[...] * alpha + jnp.sum(p, axis=0, keepdims=True)
        acc_ref[...] = acc_ref[...] * alpha + dot(vt_ref[0, :, pl.ds(off, blk)], p.astype(BF16))

    def step(j, carry):
        tile(j, False)
        return carry

    lax.fori_loop(0, i, step, 0)
    tile(i, True)
    l_val = l_ref[...]
    o = (acc_ref[...] * (1.0 / l_val)).astype(BF16)
    for h in range(group):
        o_ref[0, h * dim:(h + 1) * dim, :] = o[:, h * blk:(h + 1) * blk]
    lse_ref[0, 0] = m_ref[...] + jnp.log2(l_val)

    @pl.when(step_id == pl.num_programs(0) - 1)
    def _():
        for k in (1, 6, 7):
            ring.wait_block(order[k])
        ring.wait_sends()


class Swap:
    def __init__(self, n, src_ref, dst_ref, send_sem, recv_sem):
        self.n, self.src, self.dst, self.send_sem, self.recv_sem = n, src_ref, dst_ref, send_sem, recv_sem
        self.me = lax.axis_index('sp')

    def slot(self, dev):
        return dev % CORES * (self.n // CORES) + dev // CORES

    def peers(self):
        return [(self.me + d) % self.n for d in range(1, self.n)]

    def sends(self):
        mine = self.slot(self.me)
        return [remote(self.src.at[t], self.dst.at[mine], self.send_sem.at[d], self.recv_sem.at[mine], t)
                for d, t in enumerate(self.peers())]

    def start(self):
        for c in self.sends():
            c.start()

    def keep(self, block, sem):
        c = pltpu.make_async_copy(block, self.dst.at[self.slot(self.me)], sem)
        c.start()
        c.wait()

    def finish(self):
        for d, t in enumerate(self.peers()):
            s = self.slot(t)
            remote(self.src.at[t], self.dst.at[s], self.send_sem.at[d], self.recv_sem.at[s], t).wait_recv()
        for c in self.sends():
            c.wait_send()


def accumulate(acc_ref, lhs_ref, rhs, part, size):
    off = pl.multiple_of(part * size, size)
    acc_ref[pl.ds(off, size), :] += dot(lhs_ref[0, pl.ds(off, size), :], rhs)


def pair_sum(acc_ref, lhs_ref, rhs, got_ref, dw_ref, send_sem, recv_sem, last):
    me = lax.axis_index('sp')
    core = me % CORES
    partner = me - core + 1 - core
    size = acc_ref.shape[0] // CORES
    theirs = pl.ds(pl.multiple_of((1 - core) * size, size), size)
    mine = pl.ds(pl.multiple_of(core * size, size), size)
    copy = remote(acc_ref.at[theirs], got_ref, send_sem, recv_sem, partner)
    accumulate(acc_ref, lhs_ref, rhs, 1 - core, size)

    @pl.when(last)
    def _():
        copy.start()

    accumulate(acc_ref, lhs_ref, rhs, core, size)

    @pl.when(last)
    def _():
        copy.wait()
        dw_ref[...] = acc_ref[mine, :] + got_ref[...]


def out_grad_kernel(n, group, dim, dy_ref, w_ref, o_ref, o_hbm, do_ref, dw_ref, swap_ref, acc_ref, got_ref, keep_sem,
                    pair_send, pair_recv, send_sem, recv_sem):
    blk = dy_ref.shape[1]
    i = pl.program_id(0)
    swap = Swap(n, o_hbm, swap_ref, send_sem, recv_sem)

    @pl.when(i == 0)
    def _():
        enter(swap.peers())
        swap.start()
        acc_ref[...] = jnp.zeros_like(acc_ref)

    @pl.when(i == swap.me)
    def _():
        swap.keep(o_ref.at[0], keep_sem)

    d_o = dot(w_ref[...], dy_ref[0], NT).astype(BF16)
    for g in range(CORES):
        for h in range(group):
            row = (g * group + h) * dim
            do_ref[g, 0, :, h * blk:(h + 1) * blk] = d_o[row:row + dim]
    pair_sum(acc_ref, o_ref, dy_ref[0], got_ref, dw_ref, pair_send, pair_recv, i == n - 1)

    @pl.when(i == n - 1)
    def _():
        swap.finish()


def backward_kernel(group, dim, q_ref, do_ref, o_ref, lse_ref, k_ref, kt_ref, v_ref, cos_ref, sin_ref, out_ref,
                    dq_ref, dk_ref, dv_ref, delta_ref):
    blk = out_ref.shape[2]
    half = dim // 2
    step_id = pl.program_id(0)
    i = pl.num_programs(0) - 1 - step_id
    scale = dim ** -0.5
    c2 = scale * LOG2E

    @pl.when(step_id == 0)
    def _():
        dk_ref[...] = jnp.zeros_like(dk_ref)
        dv_ref[...] = jnp.zeros_like(dv_ref)

    dq_ref[...] = jnp.zeros_like(dq_ref)
    for h in range(group):
        prod = o_ref[0, h * dim:(h + 1) * dim, :].astype(F32) * do_ref[0, :, h * blk:(h + 1) * blk].astype(F32)
        delta_ref[:, h * blk:(h + 1) * blk] = jnp.sum(prod, axis=0, keepdims=True)

    def tile(j, masked):
        off = pl.multiple_of(j * blk, blk)
        s = dot(k_ref[pl.ds(off, blk), :], q_ref[0])
        p = jnp.exp2(s * c2 - lse_ref[0])
        if masked:
            p = jnp.where(causal_mask(s.shape[0], s.shape[1], blk), p, 0.0)
        dp = dot(v_ref[pl.ds(off, blk), :], do_ref[0]).astype(BF16).astype(F32)
        ds = (p * (dp - delta_ref[...])).astype(BF16)
        dv_ref[:, pl.ds(off, blk)] += dot(do_ref[0], p.astype(BF16), NT)
        dk_ref[:, pl.ds(off, blk)] += dot(q_ref[0], ds, NT)
        dq_ref[...] += dot(kt_ref[:, pl.ds(off, blk)], ds)

    def step(j, carry):
        tile(j, False)
        return carry

    lax.fori_loop(0, i, step, 0)
    tile(i, True)

    cos_t = cos_ref[...]
    sin_t = sin_ref[...]

    def rope_back(grad):
        grad = (grad * scale).astype(BF16).astype(F32)
        a = grad[:half]
        b = grad[half:]
        return (a * cos_t + b * sin_t).astype(BF16), (b * cos_t - a * sin_t).astype(BF16)

    for h in range(group):
        top, bottom = rope_back(dq_ref[:, h * blk:(h + 1) * blk])
        out_ref[0, h * dim:h * dim + half, :] = top
        out_ref[0, h * dim + half:(h + 1) * dim, :] = bottom
    off = pl.multiple_of(i * blk, blk)
    top, bottom = rope_back(dk_ref[:, pl.ds(off, blk)])
    base = group * dim
    out_ref[0, base:base + half, :] = top
    out_ref[0, base + half:base + dim, :] = bottom
    out_ref[0, base + dim:base + 2 * dim, :] = dv_ref[:, pl.ds(off, blk)].astype(BF16)


def weight_grad_kernel(n, g_ref, r_ref, g_hbm, dw_ref, swap_ref, acc_ref, got_ref, keep_sem, pair_send, pair_recv,
                       send_sem, recv_sem):
    i = pl.program_id(0)
    swap = Swap(n, g_hbm, swap_ref, send_sem, recv_sem)

    @pl.when(i == 0)
    def _():
        enter(swap.peers())
        swap.start()
        acc_ref[...] = jnp.zeros_like(acc_ref)

    @pl.when(i == swap.me)
    def _():
        swap.keep(g_ref.at[0], keep_sem)

    pair_sum(acc_ref, g_ref, r_ref[0], got_ref, dw_ref, pair_send, pair_recv, i == n - 1)

    @pl.when(i == n - 1)
    def _():
        swap.finish()


def spread_kernel(rows_q, dim, *refs):
    src_ref = refs[0]
    q_ref, k_ref, v_ref = refs[-3:]
    q_ref[0] = src_ref[0, :rows_q]
    k_ref[0] = src_ref[0, rows_q:rows_q + dim]
    v_ref[0] = src_ref[0, rows_q + dim:]


ANY = pl.BlockSpec(memory_space=pl.ANY)
DMA = pltpu.SemaphoreType.DMA


def call(kernel, grid, in_specs, out_specs, out_shape, name, flops, scratch=(), aliases=None, collective=None):
    params = {}
    if collective is not None:
        params = dict(collective_id=collective, has_side_effects=True)
    if grid:
        params['dimension_semantics'] = ('arbitrary',)
    return pl.pallas_call(
        kernel,
        grid=grid,
        in_specs=in_specs,
        out_specs=out_specs,
        out_shape=out_shape,
        scratch_shapes=list(scratch),
        input_output_aliases=aliases or {},
        name=name,
        cost_estimate=pl.CostEstimate(flops=int(flops), bytes_accessed=int(1e6), transcendentals=0),
        compiler_params=pltpu.CompilerParams(**params),
    )


def solution(mesh):
    n = mesh.shape['sp']
    chips = n // CORES

    def local_step(x_local, dy_local, gain, w_q, w_k, w_v, w_o):
        batch, blk, d_model = x_local.shape
        num_q, dim = w_q.shape[1], w_q.shape[2]
        num_kv = w_k.shape[1]
        assert num_kv == n and batch == CORES and chips == 4
        group = num_q // num_kv
        half = dim // 2
        seq = blk * n
        rows_q = group * dim
        rows = rows_q + 2 * dim
        cols = group * blk
        me = lax.axis_index('sp')
        chip = me // CORES
        sds = jax.ShapeDtypeStruct
        full = lambda *s: pl.BlockSpec(s, lambda i: (0,) * len(s))
        vmem = pl.BlockSpec(memory_space=pltpu.VMEM)

        wq_t = jnp.transpose(w_q, (1, 2, 0)).reshape(n, rows_q, d_model)
        wk_t = jnp.transpose(w_k, (1, 2, 0)).reshape(n, dim, d_model)
        wv_t = jnp.transpose(w_v, (1, 2, 0)).reshape(n, dim, d_model)
        w_all = jnp.concatenate([wq_t, wk_t, wv_t], axis=1)
        w_mine = lax.dynamic_slice_in_dim(w_all, chip * CORES, CORES, 0).reshape(CORES * rows, d_model)
        wo_flat = w_o.reshape(num_q * dim, d_model)
        wo_mine = lax.dynamic_slice_in_dim(wo_flat, chip * CORES * rows_q, CORES * rows_q, 0)
        cos_t, sin_t = rope_tables_t(seq, dim)
        x_hat, inv_rms, normed = norm_forward(x_local, gain)
        mm = 2.0 * seq * d_model
        att = 2.0 * seq * seq * dim * group / 2

        r_all, q_t, k, k_t, v, v_t = call(
            functools.partial(project_kernel, n, group, dim), (), [ANY, vmem, vmem, vmem],
            [ANY, vmem, vmem, vmem, vmem, vmem],
            [sds((n, blk, d_model), BF16), sds((CORES, n, dim, cols), BF16), sds((CORES, seq, dim), BF16),
             sds((CORES, dim, seq), BF16), sds((CORES, seq, dim), BF16), sds((CORES, dim, seq), BF16)],
            'project', mm * rows * 8,
            [pltpu.VMEM((blk, d_model), BF16), DMA, DMA((RING_SENDS,)), DMA((n,))],
            collective=0)(normed, w_mine, cos_t, sin_t)

        o_all, lse, dy_all = call(
            functools.partial(forward_kernel, n, group, dim, n + n - 2), (CORES * n,),
            [pl.BlockSpec((1, 1, dim, cols), lambda s: (s // n, s % n, 0, 0)),
             pl.BlockSpec((1, seq, dim), lambda s: (s // n, 0, 0)),
             pl.BlockSpec((1, dim, seq), lambda s: (s // n, 0, 0)), ANY],
            [pl.BlockSpec((1, rows_q, blk), lambda s: (s % n, s // n, 0)),
             pl.BlockSpec((1, 1, 1, cols), lambda s: (s // n, s % n, 0, 0)), ANY],
            [sds((n, CORES * rows_q, blk), BF16), sds((CORES, n, 1, cols), F32), sds((n, blk, d_model), BF16)],
            'forward', att * 16,
            [pltpu.VMEM((dim, cols), F32), pltpu.VMEM((1, cols), F32), pltpu.VMEM((1, cols), F32),
             pltpu.VMEM((blk, d_model), BF16), DMA, DMA((RING_SENDS,)), DMA((n,))],
            collective=1)(q_t, k, v_t, dy_local)

        swap_sems = [DMA, DMA, DMA, DMA((n,)), DMA((n,))]
        d_o, d_wo_mine, o_swap = call(
            functools.partial(out_grad_kernel, n, group, dim), (n,),
            [pl.BlockSpec((1, blk, d_model), lambda i: (i, 0, 0)), full(CORES * rows_q, d_model),
             pl.BlockSpec((1, CORES * rows_q, blk), lambda i: (i, 0, 0)), ANY],
            [pl.BlockSpec((CORES, 1, dim, cols), lambda i: (0, i, 0, 0)), full(rows_q, d_model), ANY],
            [sds((CORES, n, dim, cols), BF16), sds((rows_q, d_model), F32), sds((n, CORES * rows_q, blk), BF16)],
            'out_grad', mm * rows_q * 4,
            [pltpu.VMEM((CORES * rows_q, d_model), F32), pltpu.VMEM((rows_q, d_model), F32)] + swap_sems,
            collective=2)(dy_all, wo_mine, o_all, o_all)
        d_wo = lax.all_gather(d_wo_mine, 'sp', axis=0, tiled=True)

        y_proj = jnp.stack([dot(o_swap[b * chips:(b + 1) * chips].reshape(num_q * dim, blk), wo_flat, TN)
                            for b in range(batch)])
        y_out = (x_local.astype(F32) + y_proj).astype(BF16)

        w_by = w_all.reshape(chips, CORES, rows, d_model)
        d_normed = 0.0
        outs = None
        for g in range(CORES):
            rev4 = lambda a, b: pl.BlockSpec((None, 1, a, b), lambda s: (g, n - 1 - s, 0, 0))
            rev_lane = pl.BlockSpec((half, blk), lambda s: (0, n - 1 - s))
            part = lambda *s: pl.BlockSpec((None,) + s, lambda i: (g,) + (0,) * len(s))
            g_all = call(
                functools.partial(backward_kernel, group, dim), (n,),
                [rev4(dim, cols), rev4(dim, cols), pl.BlockSpec((1, rows_q, blk), lambda s: (n - 1 - s, g, 0)),
                 rev4(1, cols), part(seq, dim), part(dim, seq), part(seq, dim), rev_lane, rev_lane],
                pl.BlockSpec((1, rows, blk), lambda s: (n - 1 - s, 0, 0)), sds((n, rows, blk), BF16),
                'backward', att * 20,
                [pltpu.VMEM((dim, cols), F32), pltpu.VMEM((dim, seq), F32), pltpu.VMEM((dim, seq), F32),
                 pltpu.VMEM((1, cols), F32)])(q_t, d_o, o_all, lse, k, k_t, v, cos_t, sin_t)
            d_w_mine, g_swap = call(
                functools.partial(weight_grad_kernel, n), (n,),
                [pl.BlockSpec((1, rows, blk), lambda i: (i, 0, 0)),
                 pl.BlockSpec((1, blk, d_model), lambda i: (i, 0, 0)), ANY],
                [full(rows // CORES, d_model), ANY],
                [sds((rows // CORES, d_model), F32), sds((n, rows, blk), BF16)], 'weight_grad', mm * rows * 2,
                [pltpu.VMEM((rows, d_model), F32), pltpu.VMEM((rows // CORES, d_model), F32)] + swap_sems,
                collective=3 + g)(g_all, r_all, g_all)
            d_w = lax.all_gather(d_w_mine, 'sp', axis=0, tiled=True).reshape(chips, rows, d_model)
            first = outs is None
            outs = call(
                functools.partial(spread_kernel, rows_q, dim), (chips,),
                [pl.BlockSpec((1, rows, d_model), lambda i: (i, 0, 0))] + ([] if first else [ANY] * 3),
                [pl.BlockSpec((1, r, d_model), lambda i: (i * CORES + g, 0, 0)) for r in (rows_q, dim, dim)],
                [sds((n, r, d_model), F32) for r in (rows_q, dim, dim)], 'spread', 1e6,
                aliases=None if first else {1: 0, 2: 1, 3: 2})(d_w, *(outs or ()))
            w_g = w_by[:, g].reshape(chips * rows, d_model)
            d_normed = d_normed + jnp.stack(
                [dot(g_swap[b * chips:(b + 1) * chips].reshape(chips * rows, blk), w_g, TN) for b in range(batch)])

        d_normed = d_normed.astype(BF16).astype(F32)
        d_x_norm = norm_backward(d_normed, x_hat, inv_rms, gain)
        d_gain = lax.psum(jnp.sum(d_normed * x_hat, axis=(0, 1)), 'sp')
        d_x = (dy_local.astype(F32) + d_x_norm).astype(BF16)
        back = lambda t, h: jnp.transpose(t.reshape(h, dim, d_model), (2, 0, 1))
        return (y_out, d_x, back(outs[0], num_q), back(outs[1], num_kv), back(outs[2], num_kv),
                d_wo.reshape(num_q, dim, d_model), d_gain)

    specs_in = (P('dp', 'sp', None), P('dp', 'sp', None), P(None), P(None, None, None), P(None, None, None), P(None, None, None), P(None, None, None))
    specs_out = (P('dp', 'sp', None), P('dp', 'sp', None), P('dp', None, None), P('dp', None, None), P('dp', None, None), P('dp', None, None), P('dp'))
    return jax.shard_map(local_step, mesh=mesh, in_specs=specs_in, out_specs=specs_out, check_vma=False)
```

```python
import functools
import math
import jax
import jax.numpy as jnp
from jax import lax
from jax.experimental import pallas as pl
from jax.experimental.pallas import tpu as pltpu
from jax.sharding import PartitionSpec as P

ROPE_BASE = 1000000.0
NORM_EPS = 1e-5
LOG2E = math.log2(math.e)
NEG = -1e30
F32 = jnp.float32
BF16 = jnp.bfloat16

MESH = pl.DeviceIdType.MESH
CORES = 2

NN = (((1,), (0,)), ((), ()))
NT = (((1,), (1,)), ((), ()))
TN = (((0,), (0,)), ((), ()))


def dot(a, b, dims=NN):
    return lax.dot_general(a, b, dims, preferred_element_type=F32)


def rope_tables_t(seq_len, head_dim):
    half = head_dim // 2
    inv_freq = ROPE_BASE ** (-2.0 * jnp.arange(half, dtype=F32) / head_dim)
    angle = jnp.arange(seq_len).astype(F32)[None, :] * inv_freq[:, None]
    return jnp.cos(angle), jnp.sin(angle)


def norm_forward(x_local):
    x_f32 = x_local.astype(F32)
    inv_rms = lax.rsqrt(jnp.mean(x_f32 * x_f32, axis=-1, keepdims=True) + NORM_EPS)
    return x_f32 * inv_rms, inv_rms


def norm_backward(d_normed, x_hat, inv_rms, gain):
    d_hat = d_normed * gain
    return inv_rms * (d_hat - x_hat * jnp.mean(d_hat * x_hat, axis=-1, keepdims=True))


def remote(src, dst, send_sem, recv_sem, target):
    return pltpu.make_async_remote_copy(src_ref=src, dst_ref=dst, send_sem=send_sem, recv_sem=recv_sem,
                                        device_id={'sp': target}, device_id_type=MESH)


def enter(targets):
    barrier = pltpu.get_barrier_semaphore()
    for t in targets:
        pl.semaphore_signal(barrier, inc=1, device_id={'sp': t}, device_id_type=MESH)
    pl.semaphore_wait(barrier, len(targets))


class Ring:
    def __init__(self, n, src_ref, all_ref, send_sem, recv_sem):
        self.n, self.src, self.all, self.send_sem, self.recv_sem = n, src_ref, all_ref, send_sem, recv_sem
        me = lax.axis_index('sp')
        self.me, self.chip, self.core = me, me // CORES, me % CORES
        self.partner = self.at(0, 1 - self.core)
        self.ahead = 1 - 2 * self.core

    def at(self, hop, core):
        chips = self.n // CORES
        return (self.chip + hop + chips) % chips * CORES + core

    def neighbours(self):
        return [self.partner] + [self.at(hop, core) for hop in (1, -1) for core in range(CORES)]

    def copy(self, src, slot, k, target):
        return remote(src, self.all.at[slot], self.send_sem.at[k], self.recv_sem.at[slot], target)

    def direct(self, stage):
        hop = self.ahead if stage == 0 else -self.ahead
        b, o = self.core, 1 - self.core
        return [self.copy(self.src.at[b], self.me, 2 * stage, self.at(hop, b)),
                self.copy(self.src.at[o], self.me, 2 * stage + 1, self.at(hop, o))]

    def across(self):
        return [self.copy(self.src.at[1 - self.core], self.me, 4, self.partner)]

    def relayed(self):
        first, second = self.at(-1, 0), self.at(1, 1)
        return [self.copy(self.all.at[first], first, 5, self.at(1, self.core)),
                self.copy(self.all.at[second], second, 6, self.at(-1, self.core))]

    def wait_block(self, slot):
        self.copy(self.all.at[slot], slot, 0, self.partner).wait_recv()

    def order(self):
        b, o, a = self.core, 1 - self.core, self.ahead
        return [self.me, self.partner, self.at(-a, b), self.at(a, o), self.at(2, 0), self.at(2, 1),
                self.at(a, b), self.at(-a, o)]

    def wait_sends(self):
        for c in self.direct(0) + self.direct(1) + self.across() + self.relayed():
            c.wait_send()


RING_SENDS = 7


def start(copies):
    for c in copies:
        c.start()


def local(src, dst, sem):
    c = pltpu.make_async_copy(src, dst, sem)
    c.start()
    return c


def project_kernel(n, group, dim, x_hbm, gain_ref, wq_hbm, wk_hbm, wv_hbm, cos_ref, sin_ref, x_all, r_all, q_ref, k_ref,
                   kt_ref, v_ref, vt_ref, x_ref, r_ref, w_ref, load_sem, store_sem, w_sem, send_sem, recv_sem):
    half = dim // 2
    blk = x_ref.shape[0]
    rows_q = group * dim
    rows = rows_q + 2 * dim
    ring = Ring(n, x_hbm, x_all, send_sem, recv_sem)
    enter(ring.neighbours())
    start(ring.direct(0) + ring.across())
    weights = []
    for g in range(CORES):
        head = ring.chip * CORES + g
        weights.append(pltpu.make_async_copy(wq_hbm.at[head], w_ref.at[pl.ds(g * rows, rows_q)], w_sem))
        weights.append(pltpu.make_async_copy(wk_hbm.at[head], w_ref.at[pl.ds(g * rows + rows_q, dim)], w_sem))
        weights.append(pltpu.make_async_copy(wv_hbm.at[head], w_ref.at[pl.ds(g * rows + rows_q + dim, dim)], w_sem))
    start(weights)
    order = ring.order()

    def body(p, carry):
        slot = order[0]
        for k in range(1, n):
            slot = jnp.where(p == k, order[k], slot)

        @pl.when(p == 0)
        def _():
            local(x_hbm.at[ring.core], x_ref, load_sem).wait()

        for k in range(1, n):
            @pl.when(p == k)
            def _(k=k):
                ring.wait_block(order[k])
                if k == 3:
                    start(ring.relayed() + ring.direct(1))
                local(x_all.at[order[k]], x_ref, load_sem).wait()

        @pl.when(p > 0)
        def _():
            pltpu.make_async_copy(r_ref, r_all.at[slot], store_sem).wait()

        x = x_ref[...].astype(F32)
        inv_rms = lax.rsqrt(jnp.mean(x * x, axis=-1, keepdims=True) + NORM_EPS)
        r_ref[...] = (x * inv_rms * gain_ref[...]).astype(BF16)
        pltpu.make_async_copy(r_ref, r_all.at[slot], store_sem).start()

        @pl.when(p == 0)
        def _():
            for c in weights:
                c.wait()

        off = pl.multiple_of(slot * blk, blk)
        cos_t = cos_ref[:, pl.ds(off, blk)]
        sin_t = sin_ref[:, pl.ds(off, blk)]
        for g in range(CORES):
            lin = dot(w_ref[g * rows:(g + 1) * rows], r_ref[...], NT)
            for h in range(group):
                a = lin[h * dim:h * dim + half]
                b = lin[h * dim + half:(h + 1) * dim]
                q_ref[g, slot, :half, h * blk:(h + 1) * blk] = (a * cos_t - b * sin_t).astype(BF16)
                q_ref[g, slot, half:, h * blk:(h + 1) * blk] = (b * cos_t + a * sin_t).astype(BF16)
            a = lin[rows_q:rows_q + half]
            b = lin[rows_q + half:rows_q + dim]
            v = lin[rows_q + dim:]
            kv = jnp.concatenate([a * cos_t - b * sin_t, b * cos_t + a * sin_t, v], axis=0)
            kt_ref[g, :, pl.ds(off, blk)] = kv[:dim].astype(BF16)
            vt_ref[g, :, pl.ds(off, blk)] = v.astype(BF16)
            kv_t = kv.T.astype(BF16)
            k_ref[g, pl.ds(off, blk), :] = kv_t[:, :dim]
            v_ref[g, pl.ds(off, blk), :] = kv_t[:, dim:]
        return carry

    lax.fori_loop(0, n, body, 0)
    pltpu.make_async_copy(r_ref, r_all.at[ring.me], store_sem).wait()
    ring.wait_sends()


def causal_mask(rows, cols, blk):
    key = lax.broadcasted_iota(jnp.int32, (rows, cols), 0)
    qry = lax.broadcasted_iota(jnp.int32, (rows, cols), 1) % blk
    return key <= qry


def forward_kernel(n, group, dim, q_ref, k_ref, vt_ref, dy_hbm, o_ref, lse_ref, all_ref, acc_ref, m_ref, l_ref,
                   bounce_ref, load_sem, send_sem, recv_sem):
    blk = o_ref.shape[2]
    step_id = pl.program_id(0)
    i = step_id % n
    c2 = dim ** -0.5 * LOG2E
    ring = Ring(n, dy_hbm, all_ref, send_sem, recv_sem)
    order = ring.order()

    @pl.when(step_id == 0)
    def _():
        enter(ring.neighbours())
        start(ring.direct(0) + ring.across())
        local(dy_hbm.at[ring.core], bounce_ref, load_sem).wait()
        local(bounce_ref, all_ref.at[ring.me], load_sem)

    @pl.when(step_id == n - 2)
    def _():
        start(ring.direct(1))

    @pl.when(step_id == n)
    def _():
        ring.wait_block(order[2])
        ring.wait_block(order[3])
        start(ring.relayed())

    acc_ref[...] = jnp.zeros_like(acc_ref)
    l_ref[...] = jnp.zeros_like(l_ref)
    m_ref[...] = jnp.full_like(m_ref, NEG)

    def tile(j, masked):
        off = pl.multiple_of(j * blk, blk)
        s = dot(k_ref[0, pl.ds(off, blk), :], q_ref[0, 0])
        if masked:
            s = jnp.where(causal_mask(s.shape[0], s.shape[1], blk), s, NEG)
        m_old = m_ref[...]
        m_new = jnp.maximum(m_old, jnp.max(s, axis=0, keepdims=True) * c2)
        p = jnp.exp2(s * c2 - m_new)
        alpha = jnp.exp2(m_old - m_new)
        m_ref[...] = m_new
        l_ref[...] = l_ref[...] * alpha + jnp.sum(p, axis=0, keepdims=True)
        acc_ref[...] = acc_ref[...] * alpha + dot(vt_ref[0, :, pl.ds(off, blk)], p.astype(BF16))

    def step(j, carry):
        tile(j, False)
        return carry

    lax.fori_loop(0, i, step, 0)
    tile(i, True)
    l_val = l_ref[...]
    o = (acc_ref[...] * (1.0 / l_val)).astype(BF16)
    for h in range(group):
        o_ref[0, h * dim:(h + 1) * dim, :] = o[:, h * blk:(h + 1) * blk]
    lse_ref[0, 0] = m_ref[...] + jnp.log2(l_val)

    @pl.when(step_id == pl.num_programs(0) - 1)
    def _():
        pltpu.make_async_copy(bounce_ref, all_ref.at[ring.me], load_sem).wait()
        for k in (1, 4, 5, 6, 7):
            ring.wait_block(order[k])
        ring.wait_sends()


class Swap:
    def __init__(self, n, src_ref, dst_ref, send_sem, recv_sem):
        self.n, self.src, self.dst, self.send_sem, self.recv_sem = n, src_ref, dst_ref, send_sem, recv_sem
        self.me = lax.axis_index('sp')

    def slot(self, dev):
        return dev % CORES * (self.n // CORES) + dev // CORES

    def peers(self):
        return [(self.me + d) % self.n for d in range(1, self.n)]

    def sends(self):
        mine = self.slot(self.me)
        return [remote(self.src.at[t], self.dst.at[mine], self.send_sem.at[d], self.recv_sem.at[mine], t)
                for d, t in enumerate(self.peers())]

    def keep(self, block, sem):
        local(block, self.dst.at[self.slot(self.me)], sem).wait()

    def finish(self):
        for d, t in enumerate(self.peers()):
            s = self.slot(t)
            remote(self.src.at[t], self.dst.at[s], self.send_sem.at[d], self.recv_sem.at[s], t).wait_recv()
        for c in self.sends():
            c.wait_send()


class Spread:
    def __init__(self, n, all_ref, send_sem, recv_sem):
        self.all, self.send_sem, self.recv_sem = all_ref, send_sem, recv_sem
        self.chips = n // CORES
        me = lax.axis_index('sp')
        self.chip, self.core = me // CORES, me % CORES
        self.cut = all_ref.shape[2] // 2

    def chip_at(self, hop):
        return (self.chip + hop + self.chips) % self.chips

    def piece(self, hop, part):
        ref = self.all.at[self.chip_at(hop), self.core]
        if part is not None:
            ref = ref.at[pl.ds(part * self.cut, self.cut)]
        return ref

    def copy(self, hop, part, send, recv, to):
        ref = self.piece(hop, part)
        core = 1 - self.core if to == 0 else self.core
        return remote(ref, ref, self.send_sem.at[send], self.recv_sem.at[recv], self.chip_at(to) * CORES + core)

    def direct(self):
        return [self.copy(0, None, 0, 0, 1), self.copy(0, None, 1, 1, -1), self.copy(0, None, 2, 4, 0)]

    def relay(self):
        return [self.copy(-1, 0, 3, 2, 1), self.copy(1, 1, 4, 3, -1), self.copy(-1, None, 5, 5, 0), self.copy(1, None, 6, 6, 0)]

    def last(self):
        return [self.copy(2, 0, 7, 7, 0), self.copy(2, 1, 8, 8, 0)]

    def wait_near(self):
        self.copy(-1, None, 0, 0, 1).wait_recv()
        self.copy(1, None, 0, 1, 1).wait_recv()

    def wait_far(self):
        self.copy(2, 0, 0, 2, 1).wait_recv()
        self.copy(2, 1, 0, 3, 1).wait_recv()

    def finish(self):
        self.wait_far()
        start(self.last())
        for k, part in ((4, None), (5, None), (6, None), (7, 0), (8, 1)):
            self.copy(0, part, 0, k, 1).wait_recv()
        for c in self.direct() + self.relay() + self.last():
            c.wait_send()


SPREAD_SENDS = 9


def enter_all(n):
    me = lax.axis_index('sp')
    enter([(me + d) % n for d in range(1, n)])


def pair_sum(acc_ref, lhs, rhs, got_ref, mine_ref, send_sem, recv_sem):
    me = lax.axis_index('sp')
    core = me % CORES
    size = acc_ref.shape[0] // CORES
    halves = [pl.ds(pl.multiple_of(part * size, size), size) for part in (1 - core, core)]
    copy = remote(acc_ref.at[halves[0]], got_ref, send_sem, recv_sem, me - core + 1 - core)
    for k, rows in enumerate(halves):
        acc_ref[rows, :] += dot(lhs[rows, :], rhs)
        if k == 0:
            copy.start()
    copy.wait()
    mine_ref[...] = acc_ref[halves[1], :] + got_ref[...]


def weight_step(s, count, acc_ref, lhs_ref, rhs_ref, wide_ref, got_ref, mine_ref, pair_send, pair_recv):
    blocks, blk = lhs_ref.shape[0], lhs_ref.shape[2]
    for k in range(blocks):
        wide_ref[:, k * blk:(k + 1) * blk] = lhs_ref[k]
    rhs = rhs_ref[...].reshape(blocks * blk, rhs_ref.shape[2])

    @pl.when(s == 0)
    def _():
        acc_ref[...] = dot(wide_ref[...], rhs)

    @pl.when((s > 0) & (s < count - 1))
    def _():
        acc_ref[...] += dot(wide_ref[...], rhs)

    @pl.when(s == count - 1)
    def _():
        pair_sum(acc_ref, wide_ref, rhs, got_ref, mine_ref, pair_send, pair_recv)


def backward_step(t, n, group, dim, q_ref, do_ref, o_ref, lse_ref, k_ref, kt_ref, v_ref, cos_ref, sin_ref, out_ref,
                  dq_ref, dk_ref, dv_ref, delta_ref):
    blk = out_ref.shape[2]
    half = dim // 2
    i = n - 1 - t
    scale = dim ** -0.5
    c2 = scale * LOG2E

    @pl.when(t == 0)
    def _():
        dk_ref[...] = jnp.zeros_like(dk_ref)
        dv_ref[...] = jnp.zeros_like(dv_ref)

    dq_ref[...] = jnp.zeros_like(dq_ref)
    for h in range(group):
        prod = o_ref[0, h * dim:(h + 1) * dim, :].astype(F32) * do_ref[i, :, h * blk:(h + 1) * blk].astype(F32)
        delta_ref[:, h * blk:(h + 1) * blk] = jnp.sum(prod, axis=0, keepdims=True)

    def tile(j, masked):
        off = pl.multiple_of(j * blk, blk)
        s = dot(k_ref[pl.ds(off, blk), :], q_ref[0])
        p = jnp.exp2(s * c2 - lse_ref[0])
        if masked:
            p = jnp.where(causal_mask(s.shape[0], s.shape[1], blk), p, 0.0)
        dp = dot(v_ref[pl.ds(off, blk), :], do_ref[i]).astype(BF16).astype(F32)
        ds = (p * (dp - delta_ref[...])).astype(BF16)
        dv_ref[:, pl.ds(off, blk)] += dot(do_ref[i], p.astype(BF16), NT)
        dk_ref[:, pl.ds(off, blk)] += dot(q_ref[0], ds, NT)
        dq_ref[...] += dot(kt_ref[:, pl.ds(off, blk)], ds)

    def step(j, carry):
        tile(j, False)
        return carry

    lax.fori_loop(0, i, step, 0)
    tile(i, True)

    cos_t = cos_ref[...]
    sin_t = sin_ref[...]

    def rope_back(grad):
        grad = (grad * scale).astype(BF16).astype(F32)
        a = grad[:half]
        b = grad[half:]
        return (a * cos_t + b * sin_t).astype(BF16), (b * cos_t - a * sin_t).astype(BF16)

    for h in range(group):
        top, bottom = rope_back(dq_ref[:, h * blk:(h + 1) * blk])
        out_ref[0, h * dim:h * dim + half, :] = top
        out_ref[0, h * dim + half:(h + 1) * dim, :] = bottom
    off = pl.multiple_of(i * blk, blk)
    top, bottom = rope_back(dk_ref[:, pl.ds(off, blk)])
    base = group * dim
    out_ref[0, base:base + half, :] = top
    out_ref[0, base + half:base + dim, :] = bottom
    out_ref[0, base + dim:base + 2 * dim, :] = dv_ref[:, pl.ds(off, blk)].astype(BF16)


RELAY_AT = 5


def first_backward_kernel(n, group, dim, count, dy_ref, w_ref, o2_ref, o_hbm, q_ref, o_ref, lse_ref, k_ref, kt_ref, v_ref,
                          cos_ref, sin_ref, g_ref, do1_ref, swap_ref, dw_all, acc_ref, wide_ref, got_ref, mine_ref,
                          do_ref, dq_ref, dk_ref, dv_ref, delta_ref, sem, pair_send, pair_recv, send_sem, recv_sem,
                          spread_send, spread_recv):
    s = pl.program_id(0)
    blk = g_ref.shape[2]
    swap = Swap(n, o_hbm, swap_ref, send_sem, recv_sem)
    spread = Spread(n, dw_all, spread_send, spread_recv)
    early = n // 2 - 1

    @pl.when(s == 0)
    def _():
        enter_all(n)
        start(swap.sends()[:early])

    @pl.when(s < count)
    def _():
        weight_step(s, count, acc_ref, o2_ref, dy_ref, wide_ref, got_ref, mine_ref, pair_send, pair_recv)

    for k in range(o2_ref.shape[0]):
        @pl.when((s < count) & (s * o2_ref.shape[0] + k == swap.me))
        def _(k=k):
            swap.keep(o2_ref.at[k], sem)

    @pl.when(s == count - 1)
    def _():
        local(mine_ref, spread.piece(0, None), sem).wait()
        start(spread.direct())
        start(swap.sends()[early:])

    @pl.when((s >= count) & (s < 2 * count))
    def _():
        blocks = dy_ref.shape[0]
        d_o = dot(w_ref[...], dy_ref[...].reshape(blocks * blk, dy_ref.shape[2]), NT).astype(BF16)
        for k in range(blocks):
            i = (s - count) * blocks + k
            for h in range(group):
                do_ref[i, :, h * blk:(h + 1) * blk] = d_o[h * dim:(h + 1) * dim, k * blk:(k + 1) * blk]
                do1_ref[i, :, h * blk:(h + 1) * blk] = d_o[(group + h) * dim:(group + h + 1) * dim, k * blk:(k + 1) * blk]

    t = s - 2 * count

    @pl.when(t == RELAY_AT)
    def _():
        spread.wait_near()
        start(spread.relay())

    @pl.when(t >= 0)
    def _():
        backward_step(t, n, group, dim, q_ref, do_ref, o_ref, lse_ref, k_ref, kt_ref, v_ref, cos_ref, sin_ref, g_ref,
                      dq_ref, dk_ref, dv_ref, delta_ref)

    @pl.when(t == n - 1)
    def _():
        spread.finish()
        swap.finish()


def second_backward_kernel(n, group, dim, count, g2_ref, g_hbm, r_ref, q_ref, do_ref, o_ref, lse_ref, k_ref, kt_ref,
                           v_ref, cos_ref, sin_ref, g_ref, swap_ref, dw_all, acc_ref, wide_ref, got_ref, mine_ref,
                           dq_ref, dk_ref, dv_ref, delta_ref, sem, pair_send, pair_recv, send_sem, recv_sem,
                           spread_send, spread_recv):
    s = pl.program_id(0)
    swap = Swap(n, g_hbm, swap_ref, send_sem, recv_sem)
    spread = Spread(n, dw_all, spread_send, spread_recv)

    @pl.when(s == 0)
    def _():
        enter_all(n)
        start(swap.sends())

    @pl.when(s < count)
    def _():
        weight_step(s, count, acc_ref, g2_ref, r_ref, wide_ref, got_ref, mine_ref, pair_send, pair_recv)

    for k in range(g2_ref.shape[0]):
        @pl.when((s < count) & (s * g2_ref.shape[0] + k == swap.me))
        def _(k=k):
            swap.keep(g2_ref.at[k], sem)

    @pl.when(s == count - 1)
    def _():
        local(mine_ref, spread.piece(0, None), sem).wait()
        start(spread.direct())

    t = s - count

    @pl.when(t == RELAY_AT)
    def _():
        spread.wait_near()
        start(spread.relay())

    @pl.when(t >= 0)
    def _():
        backward_step(t, n, group, dim, q_ref, do_ref, o_ref, lse_ref, k_ref, kt_ref, v_ref, cos_ref, sin_ref, g_ref,
                      dq_ref, dk_ref, dv_ref, delta_ref)

    @pl.when(t == n - 1)
    def _():
        spread.finish()
        swap.finish()


def weight_grad_kernel(n, count, g2_ref, g_hbm, r_ref, mine_ref, swap_ref, acc_ref, wide_ref, got_ref, sem, pair_send,
                       pair_recv, send_sem, recv_sem):
    s = pl.program_id(0)
    swap = Swap(n, g_hbm, swap_ref, send_sem, recv_sem)

    @pl.when(s == 0)
    def _():
        enter_all(n)
        start(swap.sends())

    weight_step(s, count, acc_ref, g2_ref, r_ref, wide_ref, got_ref, mine_ref, pair_send, pair_recv)
    for k in range(g2_ref.shape[0]):
        @pl.when(s * g2_ref.shape[0] + k == swap.me)
        def _(k=k):
            swap.keep(g2_ref.at[k], sem)

    @pl.when(s == count - 1)
    def _():
        swap.finish()


def spread_kernel(rows_q, dim, *refs):
    src_ref = refs[0]
    q_ref, k_ref, v_ref = refs[-3:]
    q_ref[0] = src_ref[0, :rows_q]
    k_ref[0] = src_ref[0, rows_q:rows_q + dim]
    v_ref[0] = src_ref[0, rows_q + dim:]


ANY = pl.BlockSpec(memory_space=pl.ANY)
DMA = pltpu.SemaphoreType.DMA


def call(kernel, grid, in_specs, out_specs, out_shape, name, flops, scratch=(), aliases=None, collective=None):
    params = {}
    if collective is not None:
        params = dict(collective_id=collective, has_side_effects=True)
    if grid:
        params['dimension_semantics'] = ('arbitrary',)
    return pl.pallas_call(
        kernel,
        grid=grid,
        in_specs=in_specs,
        out_specs=out_specs,
        out_shape=out_shape,
        scratch_shapes=list(scratch),
        input_output_aliases=aliases or {},
        name=name,
        cost_estimate=pl.CostEstimate(flops=int(flops), bytes_accessed=int(1e6), transcendentals=0),
        compiler_params=pltpu.CompilerParams(**params),
    )


def solution(mesh):
    n = mesh.shape['sp']
    chips = n // CORES

    def local_step(x_local, dy_local, gain, w_q, w_k, w_v, w_o):
        batch, blk, d_model = x_local.shape
        num_q, dim = w_q.shape[1], w_q.shape[2]
        num_kv = w_k.shape[1]
        assert num_kv == n and batch == CORES and chips == 4
        group = num_q // num_kv
        half = dim // 2
        seq = blk * n
        rows_q = group * dim
        rows = rows_q + 2 * dim
        cols = group * blk
        count = n // 2
        me = lax.axis_index('sp')
        chip = me // CORES
        sds = jax.ShapeDtypeStruct
        full = lambda *s: pl.BlockSpec(s, lambda i: (0,) * len(s))
        vmem = pl.BlockSpec(memory_space=pltpu.VMEM)

        wq_t = jnp.transpose(w_q, (1, 2, 0)).reshape(n, rows_q, d_model)
        wk_t = jnp.transpose(w_k, (1, 2, 0)).reshape(n, dim, d_model)
        wv_t = jnp.transpose(w_v, (1, 2, 0)).reshape(n, dim, d_model)
        wo_flat = w_o.reshape(num_q * dim, d_model)
        cos_t, sin_t = rope_tables_t(seq, dim)
        mm = 2.0 * seq * d_model
        att = 2.0 * seq * seq * dim * group / 2

        _, r_all, q_t, k, k_t, v, v_t = call(
            functools.partial(project_kernel, n, group, dim), (), [ANY, vmem, ANY, ANY, ANY, vmem, vmem],
            [ANY, ANY, vmem, vmem, vmem, vmem, vmem],
            [sds((n, blk, d_model), BF16), sds((n, blk, d_model), BF16), sds((CORES, n, dim, cols), BF16),
             sds((CORES, seq, dim), BF16), sds((CORES, dim, seq), BF16), sds((CORES, seq, dim), BF16),
             sds((CORES, dim, seq), BF16)],
            'project', mm * rows * 8,
            [pltpu.VMEM((blk, d_model), BF16), pltpu.VMEM((blk, d_model), BF16), pltpu.VMEM((CORES * rows, d_model), BF16),
             DMA, DMA, DMA, DMA((RING_SENDS,)), DMA((n,))],
            collective=0)(x_local, gain.reshape(1, d_model), wq_t, wk_t, wv_t, cos_t, sin_t)

        o_all, lse, dy_all = call(
            functools.partial(forward_kernel, n, group, dim), (CORES * n,),
            [pl.BlockSpec((1, 1, dim, cols), lambda s: (s // n, s % n, 0, 0)),
             pl.BlockSpec((1, seq, dim), lambda s: (s // n, 0, 0)),
             pl.BlockSpec((1, dim, seq), lambda s: (s // n, 0, 0)), ANY],
            [pl.BlockSpec((1, rows_q, blk), lambda s: (s % n, s // n, 0)),
             pl.BlockSpec((1, 1, 1, cols), lambda s: (s // n, s % n, 0, 0)), ANY],
            [sds((n, CORES * rows_q, blk), BF16), sds((CORES, n, 1, cols), F32), sds((n, blk, d_model), BF16)],
            'forward', att * 16,
            [pltpu.VMEM((dim, cols), F32), pltpu.VMEM((1, cols), F32), pltpu.VMEM((1, cols), F32),
             pltpu.VMEM((blk, d_model), BF16), DMA, DMA((RING_SENDS,)), DMA((n,))],
            collective=1)(q_t, k, v_t, dy_local)

        def backward_specs(g, lead):
            step = lambda s: n - 1 - jnp.maximum(s - lead, 0)
            rev = lambda *s: pl.BlockSpec((None, 1) + s, lambda i: (g, step(i), 0, 0))
            part = lambda *s: pl.BlockSpec((None,) + s, lambda i: (g, 0, 0))
            lane = pl.BlockSpec((half, blk), lambda i: (0, step(i)))
            ins = dict(q=rev(dim, cols), o=pl.BlockSpec((1, rows_q, blk), lambda i: (step(i), g, 0)), lse=rev(1, cols),
                       k=part(seq, dim), kt=part(dim, seq), v=part(seq, dim), cos=lane, sin=lane)
            return ins, pl.BlockSpec((1, rows, blk), lambda i: (step(i), 0, 0))

        pair = lambda s: jnp.minimum(s, count - 1)
        back_scratch = [pltpu.VMEM((dim, cols), F32), pltpu.VMEM((dim, seq), F32), pltpu.VMEM((dim, seq), F32),
                        pltpu.VMEM((1, cols), F32)]
        sum_scratch = lambda r, out: [pltpu.VMEM((r, d_model), F32), pltpu.VMEM((r, 2 * blk), BF16),
                                      pltpu.VMEM((r // CORES, d_model), F32)] + (
                                          [pltpu.VMEM((r // CORES, d_model), F32)] if out else [])
        swap_sems = [DMA, DMA, DMA, DMA((n,)), DMA((n,))]
        spread_sems = [DMA((SPREAD_SENDS,)), DMA((SPREAD_SENDS,))]

        ins, g_spec = backward_specs(0, 2 * count)
        g_0, d_o1, o_swap, d_wo = call(
            functools.partial(first_backward_kernel, n, group, dim, count), (2 * count + n,),
            [pl.BlockSpec((2, blk, d_model), lambda s: (jnp.where(s < count, s, jnp.minimum(s - count, count - 1)), 0, 0)),
             full(CORES * rows_q, d_model), pl.BlockSpec((2, CORES * rows_q, blk), lambda s: (pair(s), 0, 0)), ANY] + list(ins.values()),
            [g_spec, full(n, dim, cols), ANY, ANY],
            [sds((n, rows, blk), BF16), sds((n, dim, cols), BF16), sds((n, CORES * rows_q, blk), BF16),
             sds((chips, CORES, rows_q, d_model), F32)],
            'backward_0', att * 20 + mm * rows_q * 4,
            sum_scratch(CORES * rows_q, True) + [pltpu.VMEM((n, dim, cols), BF16)] + back_scratch + swap_sems + spread_sems,
            collective=2)(dy_all, lax.dynamic_slice_in_dim(wo_flat, chip * CORES * rows_q, CORES * rows_q, 0), o_all, o_all,
                          q_t, o_all, lse, k, k_t, v, cos_t, sin_t)

        ins, g_spec = backward_specs(1, count)
        pair_specs = [pl.BlockSpec((2, rows, blk), lambda s: (pair(s), 0, 0)), ANY,
                      pl.BlockSpec((2, blk, d_model), lambda s: (pair(s), 0, 0))]
        ins = list(ins.values())
        g_1, g_swap0, d_w0 = call(
            functools.partial(second_backward_kernel, n, group, dim, count), (count + n,),
            pair_specs + [ins[0], full(n, dim, cols)] + ins[1:], [g_spec, ANY, ANY],
            [sds((n, rows, blk), BF16), sds((n, rows, blk), BF16), sds((chips, CORES, rows // CORES, d_model), F32)],
            'backward_1', att * 20 + mm * rows,
            sum_scratch(rows, True) + back_scratch + swap_sems + spread_sems,
            collective=3)(g_0, g_0, r_all, q_t, d_o1, o_all, lse, k, k_t, v, cos_t, sin_t)

        d_w1, g_swap1 = call(
            functools.partial(weight_grad_kernel, n, count), (count,), pair_specs, [full(rows // CORES, d_model), ANY],
            [sds((rows // CORES, d_model), F32), sds((n, rows, blk), BF16)], 'weight_grad', mm * rows,
            sum_scratch(rows, False) + swap_sems, collective=4)(g_1, g_1, r_all)
        d_w1 = lax.all_gather(d_w1, 'sp', axis=0, tiled=True)

        y_proj = jnp.stack([dot(o_swap[b * chips:(b + 1) * chips].reshape(num_q * dim, blk), wo_flat, TN)
                            for b in range(batch)])
        y_out = (x_local.astype(F32) + y_proj).astype(BF16)

        d_normed = 0.0
        outs = ()
        for g, (d_w, g_swap) in enumerate(((d_w0, g_swap0), (d_w1, g_swap1))):
            outs = call(
                functools.partial(spread_kernel, rows_q, dim), (chips,),
                [pl.BlockSpec((1, rows, d_model), lambda i: (i, 0, 0))] + [ANY] * len(outs),
                [pl.BlockSpec((1, r, d_model), lambda i: (i * CORES + g, 0, 0)) for r in (rows_q, dim, dim)],
                [sds((n, r, d_model), F32) for r in (rows_q, dim, dim)], 'spread', 1e6,
                aliases={1: 0, 2: 1, 3: 2} if outs else None)(d_w.reshape(chips, rows, d_model), *outs)
            of = lambda w: w.reshape(chips, CORES, -1, d_model)[:, g]
            w_g = jnp.concatenate([of(wq_t), of(wk_t), of(wv_t)], axis=1).reshape(chips * rows, d_model)
            d_normed = d_normed + jnp.stack(
                [dot(g_swap[b * chips:(b + 1) * chips].reshape(chips * rows, blk), w_g, TN) for b in range(batch)])

        d_normed = d_normed.astype(BF16).astype(F32)
        x_hat, inv_rms = norm_forward(x_local)
        d_x_norm = norm_backward(d_normed, x_hat, inv_rms, gain)
        d_gain = lax.psum(jnp.sum(d_normed * x_hat, axis=(0, 1)), 'sp')
        d_x = (dy_local.astype(F32) + d_x_norm).astype(BF16)
        back = lambda t, h: jnp.transpose(t.reshape(h, dim, d_model), (2, 0, 1))
        return (y_out, d_x, back(outs[0], num_q), back(outs[1], num_kv), back(outs[2], num_kv),
                d_wo.reshape(num_q, dim, d_model), d_gain)

    specs_in = (P('dp', 'sp', None), P('dp', 'sp', None), P(None), P(None, None, None), P(None, None, None), P(None, None, None), P(None, None, None))
    specs_out = (P('dp', 'sp', None), P('dp', 'sp', None), P('dp', None, None), P('dp', None, None), P('dp', None, None), P('dp', None, None), P('dp'))
    return jax.shard_map(local_step, mesh=mesh, in_specs=specs_in, out_specs=specs_out, check_vma=False)
```

```python
import functools
import math
import jax
import jax.numpy as jnp
from jax import lax
from jax.experimental import pallas as pl
from jax.experimental.pallas import tpu as pltpu
from jax.sharding import PartitionSpec as P

ROPE_BASE = 1000000.0
NORM_EPS = 1e-5
LOG2E = math.log2(math.e)
NEG = -1e30
F32 = jnp.float32
BF16 = jnp.bfloat16

MESH = pl.DeviceIdType.MESH
CORES = 2

NN = (((1,), (0,)), ((), ()))
NT = (((1,), (1,)), ((), ()))
TN = (((0,), (0,)), ((), ()))


def dot(a, b, dims=NN):
    return lax.dot_general(a, b, dims, preferred_element_type=F32)


def rope_tables_t(seq_len, head_dim):
    half = head_dim // 2
    inv_freq = ROPE_BASE ** (-2.0 * jnp.arange(half, dtype=F32) / head_dim)
    angle = jnp.arange(seq_len).astype(F32)[None, :] * inv_freq[:, None]
    return jnp.cos(angle), jnp.sin(angle)


def norm_forward(x_local):
    x_f32 = x_local.astype(F32)
    inv_rms = lax.rsqrt(jnp.mean(x_f32 * x_f32, axis=-1, keepdims=True) + NORM_EPS)
    return x_f32 * inv_rms, inv_rms


def norm_backward(d_normed, x_hat, inv_rms, gain):
    d_hat = d_normed * gain
    return inv_rms * (d_hat - x_hat * jnp.mean(d_hat * x_hat, axis=-1, keepdims=True))


def remote(src, dst, send_sem, recv_sem, target):
    return pltpu.make_async_remote_copy(src_ref=src, dst_ref=dst, send_sem=send_sem, recv_sem=recv_sem,
                                        device_id={'sp': target}, device_id_type=MESH)


def enter(targets):
    barrier = pltpu.get_barrier_semaphore()
    for t in targets:
        pl.semaphore_signal(barrier, inc=1, device_id={'sp': t}, device_id_type=MESH)
    pl.semaphore_wait(barrier, len(targets))


class Ring:
    def __init__(self, n, src_ref, all_ref, send_sem, recv_sem):
        self.n, self.src, self.all, self.send_sem, self.recv_sem = n, src_ref, all_ref, send_sem, recv_sem
        me = lax.axis_index('sp')
        self.me, self.chip, self.core = me, me // CORES, me % CORES
        self.partner = self.at(0, 1 - self.core)
        self.ahead = 1 - 2 * self.core

    def at(self, hop, core):
        chips = self.n // CORES
        return (self.chip + hop + chips) % chips * CORES + core

    def neighbours(self):
        return [self.partner] + [self.at(hop, core) for hop in (1, -1) for core in range(CORES)]

    def copy(self, src, slot, k, target):
        return remote(src, self.all.at[slot], self.send_sem.at[k], self.recv_sem.at[slot], target)

    def direct(self, stage):
        hop = self.ahead if stage == 0 else -self.ahead
        b, o = self.core, 1 - self.core
        return [self.copy(self.src.at[b], self.me, 2 * stage, self.at(hop, b)),
                self.copy(self.src.at[o], self.me, 2 * stage + 1, self.at(hop, o))]

    def across(self):
        return [self.copy(self.src.at[1 - self.core], self.me, 4, self.partner)]

    def relayed(self):
        first, second = self.at(-1, 0), self.at(1, 1)
        return [self.copy(self.all.at[first], first, 5, self.at(1, self.core)),
                self.copy(self.all.at[second], second, 6, self.at(-1, self.core))]

    def wait_block(self, slot):
        self.copy(self.all.at[slot], slot, 0, self.partner).wait_recv()

    def order(self):
        b, o, a = self.core, 1 - self.core, self.ahead
        return [self.me, self.partner, self.at(-a, b), self.at(a, o), self.at(2, 0), self.at(2, 1),
                self.at(a, b), self.at(-a, o)]

    def wait_sends(self):
        for c in self.direct(0) + self.direct(1) + self.across() + self.relayed():
            c.wait_send()


RING_SENDS = 7


def start(copies):
    for c in copies:
        c.start()


def local(src, dst, sem):
    c = pltpu.make_async_copy(src, dst, sem)
    c.start()
    return c


def causal_mask(rows, cols, blk):
    key = lax.broadcasted_iota(jnp.int32, (rows, cols), 0)
    qry = lax.broadcasted_iota(jnp.int32, (rows, cols), 1) % blk
    return key <= qry


def forward_kernel(n, group, dim, x_hbm, dy_hbm, gain_ref, wq_hbm, wk_hbm, wv_hbm, cos_ref, sin_ref, o_ref, lse_ref,
                   x_all, dy_all, r_all, q_hbm, k_hbm, kt_hbm, v_hbm, q_ref, k_ref, kt_ref, v_ref, vt_ref, x_ref, r_ref,
                   w_ref, bounce_ref, acc_ref, m_ref, l_ref, load_sem, store_sem, w_sem, out_sem, x_send, x_recv, dy_send,
                   dy_recv):
    half = dim // 2
    blk = x_ref.shape[0]
    rows_q = group * dim
    rows = rows_q + 2 * dim
    ring = Ring(n, x_hbm, x_all, x_send, x_recv)
    ring_dy = Ring(n, dy_hbm, dy_all, dy_send, dy_recv)
    order = ring.order()
    step_id = pl.program_id(0)
    s = step_id - 1
    keep = [pltpu.make_async_copy(q_ref, q_hbm, out_sem.at[0]), pltpu.make_async_copy(k_ref, k_hbm, out_sem.at[1]),
            pltpu.make_async_copy(kt_ref, kt_hbm, out_sem.at[2]), pltpu.make_async_copy(v_ref, v_hbm, out_sem.at[3]),
            pltpu.make_async_copy(bounce_ref, dy_all.at[ring.me], out_sem.at[4])]

    def project(p, carry):
        slot = order[0]
        for k in range(1, n):
            slot = jnp.where(p == k, order[k], slot)

        for k in range(1, n):
            @pl.when(p == k)
            def _(k=k):
                if k == n - 1:
                    start(ring_dy.direct(0) + ring_dy.across())
                ring.wait_block(order[k])
                if k == 3:
                    start(ring.relayed() + ring.direct(1))
                local(x_all.at[order[k]], x_ref, load_sem).wait()

        @pl.when(p > 0)
        def _():
            pltpu.make_async_copy(r_ref, r_all.at[slot], store_sem).wait()

        x = x_ref[...].astype(F32)
        inv_rms = lax.rsqrt(jnp.mean(x * x, axis=-1, keepdims=True) + NORM_EPS)
        r_ref[...] = (x * inv_rms * gain_ref[...]).astype(BF16)
        pltpu.make_async_copy(r_ref, r_all.at[slot], store_sem).start()
        off = pl.multiple_of(slot * blk, blk)
        cos_t = cos_ref[:, pl.ds(off, blk)]
        sin_t = sin_ref[:, pl.ds(off, blk)]
        for g in range(CORES):
            lin = dot(w_ref[g * rows:(g + 1) * rows], r_ref[...], NT)
            for h in range(group):
                a = lin[h * dim:h * dim + half]
                b = lin[h * dim + half:(h + 1) * dim]
                q_ref[g, slot, :half, h * blk:(h + 1) * blk] = (a * cos_t - b * sin_t).astype(BF16)
                q_ref[g, slot, half:, h * blk:(h + 1) * blk] = (b * cos_t + a * sin_t).astype(BF16)
            a = lin[rows_q:rows_q + half]
            b = lin[rows_q + half:rows_q + dim]
            v = lin[rows_q + dim:]
            kv = jnp.concatenate([a * cos_t - b * sin_t, b * cos_t + a * sin_t, v], axis=0)
            kt_ref[g, :, pl.ds(off, blk)] = kv[:dim].astype(BF16)
            vt_ref[g, :, pl.ds(off, blk)] = v.astype(BF16)
            kv_t = kv.T.astype(BF16)
            k_ref[g, pl.ds(off, blk), :] = kv_t[:, :dim]
            v_ref[g, pl.ds(off, blk), :] = kv_t[:, dim:]
        return carry

    @pl.when(step_id == 0)
    def _():
        enter(ring.neighbours())
        start(ring.direct(0) + ring.across())
        weights = []
        for g in range(CORES):
            head = ring.chip * CORES + g
            weights.append(pltpu.make_async_copy(wq_hbm.at[head], w_ref.at[pl.ds(g * rows, rows_q)], w_sem))
            weights.append(pltpu.make_async_copy(wk_hbm.at[head], w_ref.at[pl.ds(g * rows + rows_q, dim)], w_sem))
            weights.append(pltpu.make_async_copy(wv_hbm.at[head], w_ref.at[pl.ds(g * rows + rows_q + dim, dim)], w_sem))
        start(weights)
        local(x_hbm.at[ring.core], x_ref, load_sem).wait()
        for c in weights:
            c.wait()
        lax.fori_loop(0, n, project, 0)
        pltpu.make_async_copy(r_ref, r_all.at[ring.me], store_sem).wait()
        local(dy_hbm.at[ring.core], bounce_ref, load_sem).wait()
        start(keep)

    @pl.when(s == n - 2)
    def _():
        start(ring_dy.direct(1))

    @pl.when(s == n)
    def _():
        ring_dy.wait_block(order[2])
        ring_dy.wait_block(order[3])
        start(ring_dy.relayed())

    def attend():
        g = s // n
        i = s % n
        c2 = dim ** -0.5 * LOG2E
        acc_ref[...] = jnp.zeros_like(acc_ref)
        l_ref[...] = jnp.zeros_like(l_ref)
        m_ref[...] = jnp.full_like(m_ref, NEG)

        def tile(j, masked):
            off = pl.multiple_of(j * blk, blk)
            sc = dot(k_ref[g, pl.ds(off, blk), :], q_ref[g, i])
            if masked:
                sc = jnp.where(causal_mask(sc.shape[0], sc.shape[1], blk), sc, NEG)
            m_old = m_ref[...]
            m_new = jnp.maximum(m_old, jnp.max(sc, axis=0, keepdims=True) * c2)
            p = jnp.exp2(sc * c2 - m_new)
            alpha = jnp.exp2(m_old - m_new)
            m_ref[...] = m_new
            l_ref[...] = l_ref[...] * alpha + jnp.sum(p, axis=0, keepdims=True)
            acc_ref[...] = acc_ref[...] * alpha + dot(vt_ref[g, :, pl.ds(off, blk)], p.astype(BF16))

        def step(j, carry):
            tile(j, False)
            return carry

        lax.fori_loop(0, i, step, 0)
        tile(i, True)
        l_val = l_ref[...]
        o = (acc_ref[...] * (1.0 / l_val)).astype(BF16)
        for h in range(group):
            o_ref[0, h * dim:(h + 1) * dim, :] = o[:, h * blk:(h + 1) * blk]
        lse_ref[0, 0] = m_ref[...] + jnp.log2(l_val)

    pl.when(s >= 0)(attend)

    @pl.when(step_id == pl.num_programs(0) - 1)
    def _():
        for c in keep:
            c.wait()
        for k in (1, 4, 5, 6, 7):
            ring_dy.wait_block(order[k])
        ring.wait_sends()
        ring_dy.wait_sends()


class Swap:
    def __init__(self, n, src_ref, dst_ref, send_sem, recv_sem):
        self.n, self.src, self.dst, self.send_sem, self.recv_sem = n, src_ref, dst_ref, send_sem, recv_sem
        self.me = lax.axis_index('sp')

    def slot(self, dev):
        return dev % CORES * (self.n // CORES) + dev // CORES

    def peers(self):
        return [(self.me + d) % self.n for d in range(1, self.n)]

    def sends(self):
        mine = self.slot(self.me)
        return [remote(self.src.at[t], self.dst.at[mine], self.send_sem.at[d], self.recv_sem.at[mine], t)
                for d, t in enumerate(self.peers())]

    def keep(self, block, sem):
        local(block, self.dst.at[self.slot(self.me)], sem).wait()

    def finish(self):
        for d, t in enumerate(self.peers()):
            s = self.slot(t)
            remote(self.src.at[t], self.dst.at[s], self.send_sem.at[d], self.recv_sem.at[s], t).wait_recv()
        for c in self.sends():
            c.wait_send()


class Spread:
    def __init__(self, n, all_ref, send_sem, recv_sem):
        self.all, self.send_sem, self.recv_sem = all_ref, send_sem, recv_sem
        self.chips = n // CORES
        me = lax.axis_index('sp')
        self.chip, self.core = me // CORES, me % CORES
        self.ahead = 1 - 2 * self.core

    def chip_at(self, hop):
        return (self.chip + hop + self.chips) % self.chips

    def piece(self, hop):
        return self.all.at[self.chip_at(hop), self.core]

    def copy(self, hop, send, recv, to, core):
        ref = self.piece(hop)
        return remote(ref, ref, self.send_sem.at[send], self.recv_sem.at[recv], self.chip_at(to) * CORES + core)

    def ring(self, hop, send, recv, to):
        return self.copy(hop, send, recv, to, self.core)

    def across(self, hop, send, recv):
        return self.copy(hop, send, recv, 0, 1 - self.core)

    def first(self):
        return [self.ring(0, 0, 0, self.ahead), self.across(0, 1, 3)]

    def relay(self):
        return [self.ring(-self.ahead, 2, 2, self.ahead), self.across(-self.ahead, 3, 4)]

    def second(self):
        return [self.ring(0, 4, 1, -self.ahead)]

    def far(self):
        return [self.across(2, 5, 6)]

    def last(self):
        return [self.across(self.ahead, 6, 5)]

    def arrived(self, recv):
        self.ring(0, 0, recv, 0).wait_recv()

    def event(self, stage):
        if stage == 0:
            start(self.first())
        elif stage == 1:
            self.arrived(0)
            start(self.relay())
        elif stage == 2:
            start(self.second())
        elif stage == 3:
            self.arrived(2)
            start(self.far())
        else:
            self.arrived(1)
            start(self.last())
            for k in (3, 4, 5, 6):
                self.arrived(k)
            for c in self.first() + self.relay() + self.second() + self.far() + self.last():
                c.wait_send()


SPREAD_SENDS = 7


def enter_all(n):
    me = lax.axis_index('sp')
    enter([(me + d) % n for d in range(1, n)])


def pair_sum(acc_ref, lhs, rhs, got_ref, mine_ref, send_sem, recv_sem):
    me = lax.axis_index('sp')
    core = me % CORES
    size = acc_ref.shape[0] // CORES
    halves = [pl.ds(pl.multiple_of(part * size, size), size) for part in (1 - core, core)]
    copy = remote(acc_ref.at[halves[0]], got_ref, send_sem, recv_sem, me - core + 1 - core)
    for k, rows in enumerate(halves):
        acc_ref[rows, :] += dot(lhs[rows, :], rhs)
        if k == 0:
            copy.start()
    copy.wait()
    mine_ref[...] = acc_ref[halves[1], :] + got_ref[...]


def weight_step(s, count, acc_ref, lhs_ref, rhs_ref, wide_ref, got_ref, mine_ref, pair_send, pair_recv):
    blocks, blk = lhs_ref.shape[0], lhs_ref.shape[2]
    for k in range(blocks):
        wide_ref[:, k * blk:(k + 1) * blk] = lhs_ref[k]
    rhs = rhs_ref[...].reshape(blocks * blk, rhs_ref.shape[2])

    @pl.when(s == 0)
    def _():
        acc_ref[...] = dot(wide_ref[...], rhs)

    @pl.when((s > 0) & (s < count - 1))
    def _():
        acc_ref[...] += dot(wide_ref[...], rhs)

    @pl.when(s == count - 1)
    def _():
        pair_sum(acc_ref, wide_ref, rhs, got_ref, mine_ref, pair_send, pair_recv)


def backward_step(t, n, group, dim, q_ref, do_ref, o_ref, lse_ref, k_ref, kt_ref, v_ref, cos_ref, sin_ref, out_ref,
                  dq_ref, dk_ref, dv_ref, delta_ref):
    blk = out_ref.shape[2]
    half = dim // 2
    i = n - 1 - t
    scale = dim ** -0.5
    c2 = scale * LOG2E

    @pl.when(t == 0)
    def _():
        dk_ref[...] = jnp.zeros_like(dk_ref)
        dv_ref[...] = jnp.zeros_like(dv_ref)

    dq_ref[...] = jnp.zeros_like(dq_ref)
    for h in range(group):
        prod = o_ref[0, h * dim:(h + 1) * dim, :].astype(F32) * do_ref[i, :, h * blk:(h + 1) * blk].astype(F32)
        delta_ref[:, h * blk:(h + 1) * blk] = jnp.sum(prod, axis=0, keepdims=True)

    def tile(j, masked):
        off = pl.multiple_of(j * blk, blk)
        s = dot(k_ref[pl.ds(off, blk), :], q_ref[0])
        p = jnp.exp2(s * c2 - lse_ref[0])
        if masked:
            p = jnp.where(causal_mask(s.shape[0], s.shape[1], blk), p, 0.0)
        dp = dot(v_ref[pl.ds(off, blk), :], do_ref[i]).astype(BF16).astype(F32)
        ds = (p * (dp - delta_ref[...])).astype(BF16)
        dv_ref[:, pl.ds(off, blk)] += dot(do_ref[i], p.astype(BF16), NT)
        dk_ref[:, pl.ds(off, blk)] += dot(q_ref[0], ds, NT)
        dq_ref[...] += dot(kt_ref[:, pl.ds(off, blk)], ds)

    def step(j, carry):
        tile(j, False)
        return carry

    lax.fori_loop(0, i, step, 0)
    tile(i, True)

    cos_t = cos_ref[...]
    sin_t = sin_ref[...]

    def rope_back(grad):
        grad = (grad * scale).astype(BF16).astype(F32)
        a = grad[:half]
        b = grad[half:]
        return (a * cos_t + b * sin_t).astype(BF16), (b * cos_t - a * sin_t).astype(BF16)

    for h in range(group):
        top, bottom = rope_back(dq_ref[:, h * blk:(h + 1) * blk])
        out_ref[0, h * dim:h * dim + half, :] = top
        out_ref[0, h * dim + half:(h + 1) * dim, :] = bottom
    off = pl.multiple_of(i * blk, blk)
    top, bottom = rope_back(dk_ref[:, pl.ds(off, blk)])
    base = group * dim
    out_ref[0, base:base + half, :] = top
    out_ref[0, base + half:base + dim, :] = bottom
    out_ref[0, base + dim:base + 2 * dim, :] = dv_ref[:, pl.ds(off, blk)].astype(BF16)


SPREAD_STEPS = ((1, 2), (2, 4), (3, 7))


def first_backward_kernel(n, group, dim, count, dy_ref, w_hbm, o2_ref, o_hbm, q_ref, o_ref, lse_ref, k_ref, kt_ref, v_ref,
                          cos_ref, sin_ref, g_ref, do1_ref, swap_ref, dw_all, acc_ref, wide_ref, got_ref, mine_ref,
                          w_ref, w_sem, do_ref, dq_ref, dk_ref, dv_ref, delta_ref, sem, pair_send, pair_recv, send_sem, recv_sem,
                          spread_send, spread_recv):
    s = pl.program_id(0)
    blk = g_ref.shape[2]
    swap = Swap(n, o_hbm, swap_ref, send_sem, recv_sem)
    spread = Spread(n, dw_all, spread_send, spread_recv)
    early = n // 2 - 1
    w_copy = pltpu.make_async_copy(w_hbm.at[swap.me // CORES], w_ref, w_sem)

    @pl.when(s == 0)
    def _():
        enter_all(n)
        start(swap.sends()[:early])
        w_copy.start()

    @pl.when(s == count)
    def _():
        w_copy.wait()

    @pl.when(s < count)
    def _():
        weight_step(s, count, acc_ref, o2_ref, dy_ref, wide_ref, got_ref, mine_ref, pair_send, pair_recv)

    for k in range(o2_ref.shape[0]):
        @pl.when((s < count) & (s * o2_ref.shape[0] + k == swap.me))
        def _(k=k):
            swap.keep(o2_ref.at[k], sem)

    @pl.when(s == count - 1)
    def _():
        local(mine_ref, spread.piece(0), sem).wait()
        spread.event(0)
        start(swap.sends()[early:])

    @pl.when((s >= count) & (s < 2 * count))
    def _():
        blocks = dy_ref.shape[0]
        d_o = dot(w_ref[...], dy_ref[...].reshape(blocks * blk, dy_ref.shape[2]), NT).astype(BF16)
        for k in range(blocks):
            i = (s - count) * blocks + k
            for h in range(group):
                do_ref[i, :, h * blk:(h + 1) * blk] = d_o[h * dim:(h + 1) * dim, k * blk:(k + 1) * blk]
                do1_ref[i, :, h * blk:(h + 1) * blk] = d_o[(group + h) * dim:(group + h + 1) * dim, k * blk:(k + 1) * blk]

    t = s - 2 * count

    for stage, at in SPREAD_STEPS:
        @pl.when(t == at)
        def _(stage=stage):
            spread.event(stage)

    @pl.when(t >= 0)
    def _():
        backward_step(t, n, group, dim, q_ref, do_ref, o_ref, lse_ref, k_ref, kt_ref, v_ref, cos_ref, sin_ref, g_ref,
                      dq_ref, dk_ref, dv_ref, delta_ref)

    @pl.when(t == n - 1)
    def _():
        spread.event(4)
        swap.finish()


def second_backward_kernel(n, group, dim, count, g2_ref, g_hbm, r_ref, q_ref, do_ref, o_ref, lse_ref, k_ref, kt_ref,
                           v_ref, cos_ref, sin_ref, g_ref, swap_ref, dw_all, acc_ref, wide_ref, got_ref, mine_ref,
                           dq_ref, dk_ref, dv_ref, delta_ref, sem, pair_send, pair_recv, send_sem, recv_sem,
                           spread_send, spread_recv):
    s = pl.program_id(0)
    swap = Swap(n, g_hbm, swap_ref, send_sem, recv_sem)
    spread = Spread(n, dw_all, spread_send, spread_recv)

    early = n // 2 - 1

    @pl.when(s == 0)
    def _():
        enter_all(n)
        start(swap.sends()[:early])

    @pl.when(s < count)
    def _():
        weight_step(s, count, acc_ref, g2_ref, r_ref, wide_ref, got_ref, mine_ref, pair_send, pair_recv)

    for k in range(g2_ref.shape[0]):
        @pl.when((s < count) & (s * g2_ref.shape[0] + k == swap.me))
        def _(k=k):
            swap.keep(g2_ref.at[k], sem)

    @pl.when(s == count - 1)
    def _():
        local(mine_ref, spread.piece(0), sem).wait()
        spread.event(0)
        start(swap.sends()[early:])

    t = s - count

    for stage, at in SPREAD_STEPS:
        @pl.when(t == at)
        def _(stage=stage):
            spread.event(stage)

    @pl.when(t >= 0)
    def _():
        backward_step(t, n, group, dim, q_ref, do_ref, o_ref, lse_ref, k_ref, kt_ref, v_ref, cos_ref, sin_ref, g_ref,
                      dq_ref, dk_ref, dv_ref, delta_ref)

    @pl.when(t == n - 1)
    def _():
        spread.event(4)
        swap.finish()


def weight_grad_kernel(n, count, g2_ref, g_hbm, r_ref, mine_ref, swap_ref, acc_ref, wide_ref, got_ref, sem, pair_send,
                       pair_recv, send_sem, recv_sem):
    s = pl.program_id(0)
    swap = Swap(n, g_hbm, swap_ref, send_sem, recv_sem)

    @pl.when(s == 0)
    def _():
        enter_all(n)
        start(swap.sends())

    weight_step(s, count, acc_ref, g2_ref, r_ref, wide_ref, got_ref, mine_ref, pair_send, pair_recv)
    for k in range(g2_ref.shape[0]):
        @pl.when(s * g2_ref.shape[0] + k == swap.me)
        def _(k=k):
            swap.keep(g2_ref.at[k], sem)

    @pl.when(s == count - 1)
    def _():
        swap.finish()


def spread_kernel(rows_q, dim, *refs):
    src_ref = refs[0]
    q_ref, k_ref, v_ref = refs[-3:]
    q_ref[0] = src_ref[0, :rows_q]
    k_ref[0] = src_ref[0, rows_q:rows_q + dim]
    v_ref[0] = src_ref[0, rows_q + dim:]


ANY = pl.BlockSpec(memory_space=pl.ANY)
DMA = pltpu.SemaphoreType.DMA


def call(kernel, grid, in_specs, out_specs, out_shape, name, flops, scratch=(), aliases=None, collective=None):
    params = {}
    if collective is not None:
        params = dict(collective_id=collective, has_side_effects=True)
    if grid:
        params['dimension_semantics'] = ('arbitrary',)
    return pl.pallas_call(
        kernel,
        grid=grid,
        in_specs=in_specs,
        out_specs=out_specs,
        out_shape=out_shape,
        scratch_shapes=list(scratch),
        input_output_aliases=aliases or {},
        name=name,
        cost_estimate=pl.CostEstimate(flops=int(flops), bytes_accessed=int(1e6), transcendentals=0),
        compiler_params=pltpu.CompilerParams(**params),
    )


def solution(mesh):
    n = mesh.shape['sp']
    chips = n // CORES

    def local_step(x_local, dy_local, gain, w_q, w_k, w_v, w_o):
        batch, blk, d_model = x_local.shape
        num_q, dim = w_q.shape[1], w_q.shape[2]
        num_kv = w_k.shape[1]
        assert num_kv == n and batch == CORES and chips == 4
        group = num_q // num_kv
        half = dim // 2
        seq = blk * n
        rows_q = group * dim
        rows = rows_q + 2 * dim
        cols = group * blk
        count = n // 2
        sds = jax.ShapeDtypeStruct
        full = lambda *s: pl.BlockSpec(s, lambda i: (0,) * len(s))

        wq_t = jnp.transpose(w_q, (1, 2, 0)).reshape(n, rows_q, d_model)
        wk_t = jnp.transpose(w_k, (1, 2, 0)).reshape(n, dim, d_model)
        wv_t = jnp.transpose(w_v, (1, 2, 0)).reshape(n, dim, d_model)
        wo_flat = w_o.reshape(num_q * dim, d_model)
        cos_t, sin_t = rope_tables_t(seq, dim)
        mm = 2.0 * seq * d_model
        att = 2.0 * seq * seq * dim * group / 2

        at = lambda s: jnp.maximum(s - 1, 0)
        kept = [sds((CORES, n, dim, cols), BF16), sds((CORES, seq, dim), BF16), sds((CORES, dim, seq), BF16),
                sds((CORES, seq, dim), BF16)]
        blocks = sds((n, blk, d_model), BF16)
        o_all, lse, _, dy_all, r_all, q_t, k, k_t, v = call(
            functools.partial(forward_kernel, n, group, dim), (1 + CORES * n,),
            [ANY, ANY, full(1, d_model), ANY, ANY, ANY, full(half, seq), full(half, seq)],
            [pl.BlockSpec((1, rows_q, blk), lambda s: (at(s) % n, at(s) // n, 0)),
             pl.BlockSpec((1, 1, 1, cols), lambda s: (at(s) // n, at(s) % n, 0, 0))] + [ANY] * 7,
            [sds((n, CORES * rows_q, blk), BF16), sds((CORES, n, 1, cols), F32), blocks, blocks, blocks] + kept,
            'forward', att * 16 + mm * rows * 2,
            [pltpu.VMEM(t.shape, t.dtype) for t in kept] + [pltpu.VMEM((CORES, dim, seq), BF16)] +
            [pltpu.VMEM((blk, d_model), BF16)] * 2 + [pltpu.VMEM((CORES * rows, d_model), BF16), pltpu.VMEM((blk, d_model), BF16)] +
            [pltpu.VMEM((dim, cols), F32), pltpu.VMEM((1, cols), F32), pltpu.VMEM((1, cols), F32), DMA, DMA, DMA, DMA((5,)),
             DMA((RING_SENDS,)), DMA((n,)), DMA((RING_SENDS,)), DMA((n,))],
            collective=0)(x_local, dy_local, gain.reshape(1, d_model), wq_t, wk_t, wv_t, cos_t, sin_t)

        def backward_specs(g, lead):
            step = lambda s: n - 1 - jnp.maximum(s - lead, 0)
            rev = lambda *s: pl.BlockSpec((None, 1) + s, lambda i: (g, step(i), 0, 0))
            part = lambda *s: pl.BlockSpec((None,) + s, lambda i: (g, 0, 0))
            lane = pl.BlockSpec((half, blk), lambda i: (0, step(i)))
            ins = dict(q=rev(dim, cols), o=pl.BlockSpec((1, rows_q, blk), lambda i: (step(i), g, 0)), lse=rev(1, cols),
                       k=part(seq, dim), kt=part(dim, seq), v=part(seq, dim), cos=lane, sin=lane)
            return ins, pl.BlockSpec((1, rows, blk), lambda i: (step(i), 0, 0))

        pair = lambda s: jnp.minimum(s, count - 1)
        back_scratch = [pltpu.VMEM((dim, cols), F32), pltpu.VMEM((dim, seq), F32), pltpu.VMEM((dim, seq), F32),
                        pltpu.VMEM((1, cols), F32)]
        sum_scratch = lambda r, out: [pltpu.VMEM((r, d_model), F32), pltpu.VMEM((r, 2 * blk), BF16),
                                      pltpu.VMEM((r // CORES, d_model), F32)] + (
                                          [pltpu.VMEM((r // CORES, d_model), F32)] if out else [])
        swap_sems = [DMA, DMA, DMA, DMA((n,)), DMA((n,))]
        spread_sems = [DMA((SPREAD_SENDS,)), DMA((SPREAD_SENDS,))]

        ins, g_spec = backward_specs(0, 2 * count)
        g_0, d_o1, o_swap, d_wo = call(
            functools.partial(first_backward_kernel, n, group, dim, count), (2 * count + n,),
            [pl.BlockSpec((2, blk, d_model), lambda s: (jnp.where(s < count, s, jnp.minimum(s - count, count - 1)), 0, 0)),
             ANY, pl.BlockSpec((2, CORES * rows_q, blk), lambda s: (pair(s), 0, 0)), ANY] + list(ins.values()),
            [g_spec, full(n, dim, cols), ANY, ANY],
            [sds((n, rows, blk), BF16), sds((n, dim, cols), BF16), sds((n, CORES * rows_q, blk), BF16),
             sds((chips, CORES, rows_q, d_model), F32)],
            'backward_0', att * 20 + mm * rows_q * 4,
            sum_scratch(CORES * rows_q, True) + [pltpu.VMEM((CORES * rows_q, d_model), BF16), DMA, pltpu.VMEM((n, dim, cols), BF16)] + back_scratch + swap_sems + spread_sems,
            collective=2)(dy_all, wo_flat.reshape(chips, CORES * rows_q, d_model), o_all, o_all, q_t,
                          o_all, lse, k, k_t, v, cos_t, sin_t)

        ins, g_spec = backward_specs(1, count)
        pair_specs = [pl.BlockSpec((2, rows, blk), lambda s: (pair(s), 0, 0)), ANY,
                      pl.BlockSpec((2, blk, d_model), lambda s: (pair(s), 0, 0))]
        ins = list(ins.values())
        g_1, g_swap0, d_w0 = call(
            functools.partial(second_backward_kernel, n, group, dim, count), (count + n,),
            pair_specs + [ins[0], full(n, dim, cols)] + ins[1:], [g_spec, ANY, ANY],
            [sds((n, rows, blk), BF16), sds((n, rows, blk), BF16), sds((chips, CORES, rows // CORES, d_model), F32)],
            'backward_1', att * 20 + mm * rows,
            sum_scratch(rows, True) + back_scratch + swap_sems + spread_sems,
            collective=3)(g_0, g_0, r_all, q_t, d_o1, o_all, lse, k, k_t, v, cos_t, sin_t)

        d_w1, g_swap1 = call(
            functools.partial(weight_grad_kernel, n, count), (count,), pair_specs, [full(rows // CORES, d_model), ANY],
            [sds((rows // CORES, d_model), F32), sds((n, rows, blk), BF16)], 'weight_grad', mm * rows,
            sum_scratch(rows, False) + swap_sems, collective=4)(g_1, g_1, r_all)
        d_w1 = lax.all_gather(d_w1, 'sp', axis=0, tiled=True)

        y_proj = jnp.stack([dot(o_swap[b * chips:(b + 1) * chips].reshape(num_q * dim, blk), wo_flat, TN)
                            for b in range(batch)])
        y_out = (x_local.astype(F32) + y_proj).astype(BF16)

        d_normed = 0.0
        outs = ()
        for g, (d_w, g_swap) in enumerate(((d_w0, g_swap0), (d_w1, g_swap1))):
            outs = call(
                functools.partial(spread_kernel, rows_q, dim), (chips,),
                [pl.BlockSpec((1, rows, d_model), lambda i: (i, 0, 0))] + [ANY] * len(outs),
                [pl.BlockSpec((1, r, d_model), lambda i: (i * CORES + g, 0, 0)) for r in (rows_q, dim, dim)],
                [sds((n, r, d_model), F32) for r in (rows_q, dim, dim)], 'spread', 1e6,
                aliases={1: 0, 2: 1, 3: 2} if outs else None)(d_w.reshape(chips, rows, d_model), *outs)
            of = lambda w: w.reshape(chips, CORES, -1, d_model)[:, g]
            w_g = jnp.concatenate([of(wq_t), of(wk_t), of(wv_t)], axis=1).reshape(chips * rows, d_model)
            d_normed = d_normed + jnp.stack(
                [dot(g_swap[b * chips:(b + 1) * chips].reshape(chips * rows, blk), w_g, TN) for b in range(batch)])

        d_normed = d_normed.astype(BF16).astype(F32)
        x_hat, inv_rms = norm_forward(x_local)
        d_x_norm = norm_backward(d_normed, x_hat, inv_rms, gain)
        d_gain = lax.psum(jnp.sum(d_normed * x_hat, axis=(0, 1)), 'sp')
        d_x = (dy_local.astype(F32) + d_x_norm).astype(BF16)
        back = lambda t, h: jnp.transpose(t.reshape(h, dim, d_model), (2, 0, 1))
        return (y_out, d_x, back(outs[0], num_q), back(outs[1], num_kv), back(outs[2], num_kv),
                d_wo.reshape(num_q, dim, d_model), d_gain)

    specs_in = (P('dp', 'sp', None), P('dp', 'sp', None), P(None), P(None, None, None), P(None, None, None), P(None, None, None), P(None, None, None))
    specs_out = (P('dp', 'sp', None), P('dp', 'sp', None), P('dp', None, None), P('dp', None, None), P('dp', None, None), P('dp', None, None), P('dp'))
    return jax.shard_map(local_step, mesh=mesh, in_specs=specs_in, out_specs=specs_out, check_vma=False)
```
